32 devices in a mesh: section: 2 (over x), dp: 16 (over z, y, core).
Axes of the slice: x: 2, y: 2, z: 4, core: 2. Of those that a mesh axis runs over, the one named last changes fastest.
Arguments:
- activations: bfloat16 [4, 256, 4608], P('section', 'dp'), may hold values from -6 to 6
- section_sources: int32 [4], replicated, may hold values from 0 to 3, as said below
- accumulators: float32 [256, 4, 4608], P('dp', 'section'), may hold values from -6 to 6
- block_sources: int32 [256], replicated, may hold values from 0 to 255, as said below
- loss_terms: float32 [2, 16], P('section', 'dp'), may hold values from 0.35 to 6
- pre_gain: float32 [2, 4608], P('section'), may hold values from 0.1 to 1.9
- query_weight: bfloat16 [2, 4608, 2048], P('section', None, 'dp'), may hold values from -0.09375 to 0.09375
- keyval_weight: bfloat16 [2, 4608, 2048], P('section', None, 'dp'), may hold values from -0.09375 to 0.09375
- output_weight: bfloat16 [2, 2048, 4608], P('section', 'dp'), may hold values from -0.125 to 0.125
- post_gain: float32 [2, 4608], P('section'), may hold values from 0.1 to 1.9
Outputs:
- new_activations: bfloat16 [4, 256, 4608], P('section', 'dp')
- new_accumulators: float32 [256, 4, 4608], P('dp', 'section')
- check_out: bfloat16 [2, 256, 4608], P('section', 'dp')
The draws below stay inside these ranges and needn't reach their ends.
Inputs may be any that keep to these rules, and one draw needn't show every extreme that they name: `section_sources`: A permutation; each old section's micro-batches fill 1 slots of each new section. `block_sources`: A permutation; each old data index's blocks fill 1 block of each new data index.
All inputs are finite; a program needn't handle non-finite values.
Results may differ from the reference program's by a relative error of at most 0.014.
Values may be sent and summed in bfloat16 or wider, within the bound.
A program may use at most 64 MiB of HBM per device.

```python
import jax
import jax.numpy as jnp
from jax import lax

D = 4608
HD = 128
HEADS = 16
KV_HEADS = 8
TOKENS = 256
MB_DEV = 2
MB_ALL = 4
BROWS = 2
BLK_DEV = 16
BLOCKS = 256
ACC_ROWS = 4
N_SECTION = 2
N_DP = 16


def balanced_sources(key, groups, per_group):
    per_peer = per_group // groups

    def source_order(which):
        return jax.random.permutation(jax.random.fold_in(key, which), per_group)
    orders = jax.vmap(source_order)(jnp.arange(groups, dtype=jnp.int32))
    sources = jnp.arange(groups, dtype=jnp.int32)[:, None] * per_group + orders.astype(jnp.int32)
    chosen = sources.reshape(groups, groups, per_peer).transpose(1, 0, 2).reshape(groups, per_group)

    def shuffle(which, entries):
        return jax.random.permutation(jax.random.fold_in(key, 100000 + which), entries)
    table = jax.vmap(shuffle)(jnp.arange(groups, dtype=jnp.int32), chosen)
    return table.reshape(-1).astype(jnp.int32)


def draw_section_sources(key, part):
    return balanced_sources(jax.random.fold_in(key, 11), N_SECTION, MB_DEV)


def draw_block_sources(key, part):
    return balanced_sources(jax.random.fold_in(key, 23), N_DP, BLK_DEV)


def draw_loss_terms(key, part):
    rising = 1.0 + 2.0 * jnp.arange(N_DP, dtype=jnp.float32) / (N_DP - 1)
    subkey = jax.random.fold_in(key, 37)
    factor = jnp.exp(jax.random.uniform(subkey, (N_SECTION, N_DP), jnp.float32, jnp.log(0.7), jnp.log(1.4)))
    return (rising[None, :] * factor).astype(jnp.float32)


def shard_levels(stream_key, extent, shards, smallest, top_value):
    loudness, own = 1.0, jax.random.fold_in(stream_key, 6)
    for axis_at, blocks in shards:
        steps = jnp.exp(jax.random.uniform(jax.random.fold_in(own, axis_at), (blocks,), jnp.float32, smallest / len(shards), top_value / len(shards)))
        loudness = loudness * jnp.repeat(steps, extent[axis_at] // blocks).reshape([-1 if axis == axis_at else 1 for axis in range(len(extent))])
    return loudness


def bell_draw(rng, extent, spread, reach, shards=(), held_as=jnp.bfloat16):
    values = jax.random.normal(rng, extent, jnp.float32) * spread
    if len(shards) > 0:
        values = shard_levels(rng, extent, shards, -0.22, 0.18) * values
    return jnp.clip(values, min=-reach, max=reach).astype(held_as)


def setup_inputs(seed: int = 0) -> dict:
    seeds = jax.random.split(jax.random.key(seed), 11)
    activations = bell_draw(seeds[0], (MB_ALL, TOKENS, D), 1.0, 6.0, ((0, 2), (1, 16)))
    section_sources = draw_section_sources(jax.random.fold_in(seeds[10], 71), 0)
    accumulators = bell_draw(seeds[2], (BLOCKS, ACC_ROWS, D), 1.0, 6.0, ((0, 16), (1, 2)), jnp.float32)
    block_sources = draw_block_sources(jax.random.fold_in(seeds[10], 71), 0)
    loss_terms = draw_loss_terms(jax.random.fold_in(seeds[10], 71), 0)
    pre_gain = jnp.clip(1.0 + 0.18 * jax.random.normal(seeds[5], (N_SECTION, D), jnp.float32), 0.1, 1.9)
    query_weight = bell_draw(seeds[6], (N_SECTION, D, HEADS * HD), D ** -0.5, 0.09375, ((0, 2), (2, 16)))
    keyval_weight = bell_draw(seeds[7], (N_SECTION, D, HEADS * HD), D ** -0.5, 0.09375, ((0, 2), (2, 16)))
    output_weight = bell_draw(seeds[8], (N_SECTION, HEADS * HD, D), (HEADS * HD) ** -0.5, 0.125, ((0, 2), (1, 16)))
    post_gain = jnp.clip(1.0 + 0.18 * jax.random.normal(seeds[9], (N_SECTION, D), jnp.float32), 0.1, 1.9)
    return dict(activations=activations, section_sources=section_sources, accumulators=accumulators, block_sources=block_sources, loss_terms=loss_terms, pre_gain=pre_gain, query_weight=query_weight, keyval_weight=keyval_weight, output_weight=output_weight, post_gain=post_gain)


def rms_norm(values, gain):
    meansq = lax.optimization_barrier(jnp.mean(values * values, axis=-1, keepdims=True))
    return values * lax.rsqrt(meansq + 1e-06) * gain

def rotary(values, positions):
    width = values.shape[-1]
    middle = width // 2
    counter = jnp.arange(middle, dtype=jnp.float32)
    freqs = 10000.0 ** (-2.0 * counter / width)
    angles = positions.astype(jnp.float32)[:, None] * freqs[None, :]
    cosine = jnp.cos(angles)
    sine = jnp.sin(angles)
    if values.ndim == 3:
        cosine = cosine[:, None, :]
        sine = sine[:, None, :]
    first = values[..., :middle]
    second = values[..., middle:]
    return jnp.concatenate([first * cosine - second * sine, second * cosine + first * sine], axis=-1)

def check_layer(checked, gain_pre, w_query, w_keyval, w_output, gain_post):
    length = checked.shape[0]
    positions = jnp.arange(length, dtype=jnp.int32)
    normed = rms_norm(checked.astype(jnp.float32), gain_pre).astype(jnp.bfloat16)
    queries = jnp.dot(normed, w_query, preferred_element_type=jnp.float32).reshape(length, HEADS, HD)
    keyvals = jnp.dot(normed, w_keyval, preferred_element_type=jnp.float32).reshape(length, KV_HEADS, 2, HD)
    queries = rotary(queries, positions).astype(jnp.bfloat16)
    key_rows = rotary(keyvals[:, :, 0, :], positions).astype(jnp.bfloat16)
    value_rows = keyvals[:, :, 1, :].astype(jnp.bfloat16)
    key_rows = jnp.repeat(key_rows, 2, axis=1)
    value_rows = jnp.repeat(value_rows, 2, axis=1)
    scale_factor = (D / HEADS) ** (-0.5)
    scores = jnp.einsum('qhd,khd->hqk', queries.astype(jnp.float32), key_rows.astype(jnp.float32)) * scale_factor
    capped = 50.0 * jnp.tanh(scores / 50.0)
    causal = positions[None, :] <= positions[:, None]
    expd = jnp.where(causal[None, :, :], jnp.exp(capped), 0.0)
    denominator = lax.optimization_barrier(jnp.sum(expd, axis=-1))
    probs = expd.astype(jnp.bfloat16)
    numer = jnp.einsum('hqk,khd->hqd', probs.astype(jnp.float32), value_rows.astype(jnp.float32))
    attended = (numer / denominator[:, :, None]).astype(jnp.bfloat16)
    attended = jnp.transpose(attended, (1, 0, 2)).reshape(length, HEADS * HD)
    summed = jnp.dot(attended, w_output, preferred_element_type=jnp.float32)
    return (checked.astype(jnp.float32) + rms_norm(summed, gain_post)).astype(jnp.bfloat16)

def reference(activations, section_sources, accumulators, block_sources, loss_terms, pre_gain, query_weight, keyval_weight, output_weight, post_gain):
    moved = jnp.take(activations, section_sources, axis=0)
    regrouped = jnp.take(accumulators, block_sources, axis=0)
    totals = lax.optimization_barrier(jnp.sum(loss_terms, axis=1))
    factor = N_DP / totals
    scaled = regrouped.reshape(BLOCKS, N_SECTION, BROWS, D) * factor[None, :, None, None]
    new_accumulators = scaled.reshape(BLOCKS, ACC_ROWS, D)
    checks = []
    for section_id in range(N_SECTION):
        checks.append(check_layer(moved[section_id * MB_DEV], pre_gain[section_id], query_weight[section_id], keyval_weight[section_id], output_weight[section_id], post_gain[section_id]))
    return (moved, new_accumulators, jnp.stack(checks, axis=0))
```

```python
import functools

import jax
import jax.numpy as jnp
import numpy as np
from jax import lax
from jax.experimental import pallas as pl
from jax.experimental.pallas import tpu as pltpu
from jax.sharding import PartitionSpec as P

LANES = 128
VMEM_BYTES = 67043328
CHUNKS = 6
MIXED = (0, 3, 1, 4, 2, 5)
AHEAD = ((0, 1, 3, 2, 4, 5), (3, 0, 4, 1, 5, 2))
SORTED = ((0, 1, 2, 3, 4, 5), (3, 4, 5, 0, 1, 2))
F32 = jnp.float32
BF16 = jnp.bfloat16


def pick(table, own, groups, per_group, peer, rank):
    def visit(j, carry):
        seen, found = carry
        source = table[peer * per_group + j]
        mine = (source // per_group == own).astype(jnp.int32)
        hit = mine * (seen == rank).astype(jnp.int32)
        return seen + mine, found + hit * (source % per_group)

    zero = jnp.int32(0)
    return lax.fori_loop(0, per_group, visit, (zero, zero), unroll=True)[1]


def origin(table, own, per_group, per_peer, entry):
    owner = table[own * per_group + entry] // per_group
    if per_peer == 1:
        return owner, 0

    def visit(j, seen):
        same = table[own * per_group + j] // per_group == owner
        return seen + same.astype(jnp.int32) * (j < entry).astype(jnp.int32)

    return owner, lax.fori_loop(0, per_group, visit, jnp.int32(0))


def rotary_tables(length, width):
    half = width // 2
    freqs = np.float32(10000.0) ** (np.float32(-2.0) * np.arange(half, dtype=np.float32) / np.float32(width))
    angles = np.arange(length, dtype=np.float32)[:, None] * freqs.astype(np.float32)[None, :]
    cosine, sine = np.cos(angles.astype(np.float64)), np.sin(angles.astype(np.float64))
    return np.stack(
        [np.concatenate([cosine, cosine], 1), np.concatenate([-sine, sine], 1)]
    ).astype(np.float32)


def kernel(
    dims,
    secs_hbm, blks_hbm, loss_hbm, act_hbm, acc_hbm, pre_hbm, wq_hbm, wkv_hbm, wo_hbm, post_hbm, rot_hbm,
    moved, accout, outbuf,
    secs, blks, loss, act, acc, pre, post, rot, turn, w, wo,
    stage, actrecv, sacc, racc,
    gath, qs, kvs, part, ring_in, ring_out,
    load_sem, act_out, act_sem, w_sem, wq_sem, wo_sem, blk_sem, ag_out, ag_sem, fwd_sem, ring_done, ring_sem,
):
    n_sec, n_dp = dims
    mb, toks, d = act.shape
    blk, brows, _ = acc.shape
    act_pp, blk_pp = mb // n_sec, blk // n_dp
    chips = n_dp // 2
    far = chips // 2
    kd = d // CHUNKS
    length = n_dp * toks
    hd = wq_hbm.shape[2]
    sec, me = lax.axis_index("section"), lax.axis_index("dp")
    core, chip = me % 2, me // 2
    side, rung = chip % 2, chip // 2
    pos = rung * (1 - side) + (chips - 1 - rung) * side

    def chip_at(p):
        q = (p + 2 * chips) % chips
        s = q // (chips // 2)
        return 2 * (q * (1 - s) + (chips - 1 - q) * s) + s

    def device(p):
        return {"dp": 2 * chip_at(p) + core}

    partner = {"dp": me + 1 - 2 * core}

    def remote(src, dst, send_sem, recv_sem, dev):
        return pltpu.make_async_remote_copy(
            src_ref=src, dst_ref=dst, send_sem=send_sem, recv_sem=recv_sem,
            device_id=dev, device_id_type=pl.DeviceIdType.MESH,
        )

    barrier = pltpu.get_barrier_semaphore()
    for o in range(1, n_sec):
        pl.semaphore_signal(barrier, inc=1, device_id={"section": (sec + o) % n_sec},
                            device_id_type=pl.DeviceIdType.MESH)
    for near in (device(pos + 1), device(pos - 1), partner):
        pl.semaphore_signal(barrier, inc=1, device_id=near, device_id_type=pl.DeviceIdType.MESH)

    kv_cols = pl.ds(pl.multiple_of(2 * hd + core * hd, LANES), hd)
    q_cols = pl.ds(pl.multiple_of(core * hd, LANES), hd)
    wo_rows = pl.ds(pl.multiple_of(core * hd, LANES), hd)
    names = ("secs", "act", "pre", "wkv", "wo", "blks", "loss", "acc", "wq", "rot", "post")
    pairs = [
        (secs_hbm, secs), (act_hbm, act), (pre_hbm, pre), (wkv_hbm.at[0], w.at[:, kv_cols]),
        (wo_hbm.at[0], wo.at[wo_rows]), (blks_hbm, blks), (loss_hbm, loss), (acc_hbm, acc),
        (wq_hbm.at[0], w.at[:, q_cols]), (rot_hbm, rot), (post_hbm, post),
    ]
    loads = {
        name: pltpu.make_async_copy(src, dst, load_sem.at[i])
        for i, (name, (src, dst)) in enumerate(zip(names, pairs))
    }
    for name in names:
        loads[name].start()

    loads["secs"].wait()
    loads["act"].wait()
    for q in range(n_sec):
        for r in range(act_pp):
            block = act[pick(secs, sec, n_sec, mb, q, r)]
            for k in range(CHUNKS):
                stage[q, k, r] = block[:, k * kd:(k + 1) * kd]
    pl.semaphore_wait(barrier, n_sec - 1 + 3)
    act_copies = [[] for _ in range(CHUNKS)]
    for k in MIXED:
        for o in range(1, n_sec):
            q = (sec + o) % n_sec
            copy = remote(stage.at[q, k], actrecv[k].at[sec], act_out.at[o - 1], act_sem.at[o - 1, k], {"section": q})
            copy.start()
            act_copies[k].append(copy)
    for k in range(CHUNKS):
        actrecv[k][sec] = stage[sec, k]

    loads["wkv"].wait()
    loads["wo"].wait()
    loads["wq"].wait()

    def whole(ref, sems):
        return remote(ref, ref, sems.at[0], sems.at[1], partner)

    kv_copy, q_copy = whole(w.at[:, kv_cols], w_sem), whole(w.at[:, q_cols], wq_sem)
    wo_copy = whole(wo.at[wo_rows], wo_sem)

    def share(ref, sems):
        remote(ref, ref, sems.at[0], sems.at[1], partner).start()

    for name in ("acc", "blks", "loss"):
        loads[name].wait()
    term = jnp.full((brows, LANES), loss[0, 0], F32)
    high = term.astype(BF16).astype(F32)
    lane = lax.broadcasted_iota(jnp.int32, (brows, LANES), 1)
    row = lax.broadcasted_iota(jnp.int32, (brows, LANES), 0)
    tail = jnp.where(row > 0, 0.0, jnp.where(lane == 0, high, jnp.where(lane == 1, term - high, 0.0)))

    def pack(p, carry):
        for r in range(blk_pp):
            sacc[p, r, :, pl.ds(0, d)] = acc[pick(blks, me, n_dp, blk, p, r)].astype(BF16)
            sacc[p, r, :, pl.ds(d, LANES)] = tail.astype(BF16)
        return carry

    lax.fori_loop(0, n_dp // 2, pack, 0)
    loads["pre"].wait()

    def hops(way, k):
        return far if (k < CHUNKS // 2) == (way == 0) else far - 1

    step_of = (1, -1)

    def width(k):
        return kd + LANES if k == MIXED[-1] else kd

    def slot(way, hop):
        return 0 if hop == 0 else min(2 * hop - 1 + way, chips - 1)

    def blocks_of(k, c, slots):
        return gath.at[k, c, slots, :, pl.ds(0, width(k))]

    def gather_copy(way, hop, k):
        return remote(blocks_of(k, core, slot(way, hop - 1)), blocks_of(k, core, slot(way, hop)),
                      ag_out.at[k], ag_sem.at[way, hop - 1, k], device(pos + step_of[way]))

    near = 2 * (far - 2) + 1
    spans = (slice(0, near), slice(near, chips))

    def pass_on(j, k):
        block = blocks_of(k, core, j)
        remote(block, block, fwd_sem.at[0, k], fwd_sem.at[1 if j < near else 2, k], partner).start()

    square = jnp.zeros((toks, 1), F32)
    for k in MIXED:
        for copy in act_copies[k]:
            copy.wait_recv()
        owner, number = origin(secs, sec, mb, act_pp, 0)
        piece = actrecv[k][owner, number].astype(F32)
        square = square + jnp.sum(piece * piece, axis=-1, keepdims=True)
        gath[k, core, 0, :, pl.ds(0, kd)] = (piece * pre[:, k * kd:(k + 1) * kd]).astype(BF16)
        if k == MIXED[-1]:
            root = jnp.broadcast_to(lax.rsqrt(square / d + 1e-06), (toks, LANES))
            high = root.astype(BF16).astype(F32)
            lane = lax.broadcasted_iota(jnp.int32, (toks, LANES), 1)
            gath[k, core, 0, :, pl.ds(kd, LANES)] = jnp.where(
                lane == 0, high, jnp.where(lane == 1, root - high, 0.0)).astype(BF16)
        for way in range(2):
            gather_copy(way, 1, k).start()
        pass_on(0, k)

    other = me + 1 - 2 * core

    def project(k, part_of, fresh):
        span = spans[part_of]
        count = span.stop - span.start

        def add(ref, index, rows, cols):
            rows = rows.reshape(-1, kd)
            terms = jnp.dot(rows, w[k * kd:(k + 1) * kd, cols], preferred_element_type=F32)
            terms = terms.reshape(ref[index].shape)
            ref[index] = terms if fresh else ref[index] + terms

        add(qs, span, gath[k, core, span, :, pl.ds(0, kd)], slice(0, 2 * hd))
        block = blocks_of(k, 1 - core, pl.ds(span.start, count))
        remote(block, block, fwd_sem.at[0, k], fwd_sem.at[1 + part_of, k], partner).wait_recv()
        add(kvs, (slice(None), span), gath[k, :, span, :, pl.ds(0, kd)], slice(2 * hd, 4 * hd))

    def send_block(peer):
        remote(sacc.at[peer], racc.at[me], blk_sem.at[0], blk_sem.at[1], {"dp": peer}).start()

    def send_blocks(places):
        for way, hop in places:
            for c in range(2):
                send_block(2 * chip_at(pos + step_of[way] * hop) + (core + c) % 2)

    loads["rot"].wait()
    for j in range(chips):
        place = chip_at(pos + (j + 1) // 2 * (1 - 2 * (j % 2)))
        for c in range(2):
            for t in range(2):
                turn[t, c, j] = rot[t, place, c]

    half = CHUNKS // 2
    quarter = n_dp // 8
    for hop in range(1, far + 1):
        order = AHEAD if hop == 1 else SORTED
        for i in range(CHUNKS if hop < far else half):
            for way in range(2):
                k = order[way][i]
                gather_copy(way, hop, k).wait_recv()
                if hop < hops(way, k):
                    gather_copy(way, hop + 1, k).start()
                pass_on(slot(way, hop), k)
            if hop == 1:
                rows = pl.ds(i * kd, kd)
                share(w.at[rows, kv_cols], w_sem)
                share(w.at[rows, q_cols], wq_sem)
                if i < 4:
                    lax.fori_loop((4 + i) * quarter, (5 + i) * quarter, pack, 0)
                elif i == 4:
                    racc[me] = sacc[me]
                    send_block(other)
            if hop == 2:
                share(wo.at[wo_rows, pl.ds(i * kd, kd)], wo_sem)
            if hop == far - 1 and i == 1:
                kv_copy.wait_recv()
                q_copy.wait_recv()
            if hop == far - 1 and i > 0:
                project(i - 1, 0, i == 1)
            if hop == far and i > 0:
                project(i - 1, 1, i == 1)
                project(half + i - 1, 1, False)
        if hop == far - 1:
            send_blocks([(way, h) for h in range(1, far) for way in range(2)])
            project(CHUNKS - 1, 0, False)
    send_blocks([(0, far)])
    project(half - 1, 1, False)
    project(CHUNKS - 1, 1, False)

    def root_of(parts):
        return jnp.sum(parts.reshape(-1, LANES).astype(F32), axis=-1, keepdims=True)

    def turned(v, tables, root):
        return (v * (tables[0].reshape(-1, hd) * root) + pltpu.roll(v, hd // 2, 1) * (tables[1].reshape(-1, hd) * root)).astype(BF16)

    mine = chips * toks
    root = root_of(gath[CHUNKS - 1, :, :, :, pl.ds(kd, LANES)])
    own_root = root_of(gath[CHUNKS - 1, core, :, :, pl.ds(kd, LANES)])
    own_turn = turn[0, core], turn[1, core]

    def token_at(row, first_core):
        block = row // toks
        j = block % chips
        p = (pos + (j + 1) // 2 * (1 - 2 * (j % 2)) + 2 * chips) % chips
        s = p // (chips // 2)
        return (2 * (2 * (p * (1 - s) + (chips - 1 - p) * s) + s) + first_core + block // chips) * toks + row % toks

    q_rows = qs[...].reshape(mine, 2 * hd)
    kv_rows = kvs[...].reshape(length, 2 * hd)
    queries = jnp.concatenate([turned(q_rows[:, 0:hd], own_turn, own_root), turned(q_rows[:, hd:2 * hd], own_turn, own_root)], axis=0)
    keys = turned(kv_rows[:, 0:hd], (turn[0], turn[1]), root)
    values = (kv_rows[:, hd:2 * hd] * root).astype(BF16)
    scores = lax.dot_general(queries, keys, (((1,), (1,)), ((), ())), preferred_element_type=F32)
    scores = scores * ((d / n_dp) ** (-0.5) / 50.0)
    query_token = token_at(lax.broadcasted_iota(jnp.int32, (2 * mine, 1), 0) % mine, core)
    key_token = token_at(lax.broadcasted_iota(jnp.int32, (1, length), 1), 0)
    expd = jnp.where(key_token <= query_token, jnp.exp(50.0 * jnp.tanh(scores)), 0.0)
    denominator = jnp.sum(expd, axis=-1, keepdims=True)
    numer = jnp.dot(expd.astype(BF16), values, preferred_element_type=F32)
    attended = (numer / denominator).astype(BF16)
    both = jnp.concatenate([attended[0:mine], attended[mine:2 * mine]], axis=1)
    wo_copy.wait_recv()

    def ring_copy(way, step, k):
        return remote(ring_out.at[k, way * far + step - 1], ring_in.at[k, way * far + step - 1],
                      ring_done.at[k], ring_sem.at[way, step - 1, k], device(pos + step_of[way]))

    for k in range(CHUNKS):
        terms = jnp.dot(both, wo[:, k * kd:(k + 1) * kd], preferred_element_type=F32)
        part[k] = terms.reshape(chips, toks, kd)
        for way in range(2):
            ring_out[k, way * far] = part[k, slot(1 - way, hops(way, k))].astype(BF16)
            ring_copy(way, 1, k).start()
    for j in range(mb):
        owner, number = origin(secs, sec, mb, act_pp, j)
        for k in range(CHUNKS):
            moved[j, :, k * kd:(k + 1) * kd] = actrecv[k][owner, number]

    others = pl.ds(0, n_dp - 1)
    all_blocks = remote(sacc.at[others], racc.at[others], blk_sem.at[0], blk_sem.at[1], partner)
    all_blocks.wait_recv()
    scale_sum = jnp.sum(racc[:, 0, :, pl.ds(d, LANES)].astype(F32), axis=0)
    factor = n_dp / jnp.sum(jnp.sum(scale_sum, axis=0, keepdims=True), axis=1, keepdims=True)

    def unpack(b, carry):
        owner, number = origin(blks, me, blk, blk_pp, b)
        accout[b] = racc[owner, number, :, pl.ds(0, d)].astype(F32) * factor
        return carry

    lax.fori_loop(0, blk, unpack, 0)

    for step in range(1, far):
        for k in range(CHUNKS):
            for way in range(2):
                left = hops(way, k) - step
                if left < 1:
                    continue
                ring_copy(way, step, k).wait_recv()
                total = part[k, slot(1 - way, left)] + ring_in[k, way * far + step - 1].astype(F32)
                ring_out[k, way * far + step] = total.astype(BF16)
                ring_copy(way, step + 1, k).start()

    pieces = []
    for k in range(CHUNKS):
        total = part[k, 0]
        for way in range(2):
            step = hops(way, k)
            ring_copy(way, step, k).wait_recv()
            total = total + ring_in[k, way * far + step - 1].astype(F32)
        pieces.append(total)
    loads["post"].wait()
    square = sum(jnp.sum(t * t, axis=-1, keepdims=True) for t in pieces)
    scale = lax.rsqrt(square / d + 1e-06)
    for k in range(CHUNKS):
        cols = slice(k * kd, (k + 1) * kd)
        outbuf[0, :, cols] = (
            moved[0, :, cols].astype(F32) + pieces[k] * scale * post[:, cols]
        ).astype(BF16)
    for copy in (kv_copy, q_copy, wo_copy, all_blocks):
        copy.wait_send()
    for o in range(1, n_sec):
        q = (sec + o) % n_sec
        remote(stage.at[q], stage.at[q], act_out.at[o - 1], act_sem.at[o - 1, 0], {"section": q}).wait_send()
    for k in range(CHUNKS):
        for places, sem in ((slice(None), fwd_sem.at[0, k]), (pl.ds(0, chips - 1), ag_out.at[k])):
            block = blocks_of(k, core, places)
            remote(block, block, sem, fwd_sem.at[1, k], partner).wait_send()
        block = ring_out.at[k, pl.ds(0, chips - 1)]
        remote(block, block, ring_done.at[k], fwd_sem.at[1, k], partner).wait_send()


def write_out(moved, accout, outbuf, moved_hbm, newacc_hbm, check_hbm, sems):
    copies = [
        pltpu.make_async_copy(src, dst, sems.at[i])
        for i, (src, dst) in enumerate([(accout, newacc_hbm), (moved, moved_hbm), (outbuf, check_hbm)])
    ]
    for copy in copies:
        copy.start()
    for copy in copies:
        copy.wait()


def make_on_device(n_sec, n_dp):
    def on_device(activations, section_sources, accumulators, block_sources, loss_terms,
                  pre_gain, query_weight, keyval_weight, output_weight, post_gain):
        mb, toks, d = activations.shape
        blk, brows, _ = accumulators.shape
        hd = query_weight.shape[2]
        chips, far, kd, length = n_dp // 2, n_dp // 4, d // CHUNKS, n_dp * toks
        rot = jnp.asarray(rotary_tables(length, hd).reshape(2, chips, 2, toks, hd))
        smem = pltpu.SMEM
        in_hbm = pl.BlockSpec(memory_space=pltpu.HBM)
        vmem = pl.BlockSpec(memory_space=pltpu.VMEM)
        dma = pltpu.SemaphoreType.DMA
        act_pp, blk_pp = mb // n_sec, blk // n_dp
        out_bytes = activations.size * 2 + accumulators.size * 4 + toks * d * 2
        held = pl.pallas_call(
            functools.partial(kernel, (n_sec, n_dp)),
            out_shape=(
                pltpu.VMEM(activations.shape, BF16),
                pltpu.VMEM(accumulators.shape, F32),
                pltpu.VMEM((1, toks, d), BF16),
            ),
            in_specs=[in_hbm] * 11,
            out_specs=(vmem,) * 3,
            scratch_shapes=[
                smem(section_sources.shape, jnp.int32),
                smem(block_sources.shape, jnp.int32),
                smem((1, 1), F32),
                pltpu.VMEM(activations.shape, BF16),
                pltpu.VMEM(accumulators.shape, F32),
                pltpu.VMEM((1, d), F32),
                pltpu.VMEM((1, d), F32),
                pltpu.VMEM(rot.shape, F32),
                pltpu.VMEM((2, 2, chips, toks, hd), F32),
                pltpu.VMEM((d, 4 * hd), BF16),
                pltpu.VMEM((2 * hd, d), BF16),
                pltpu.VMEM((n_sec, CHUNKS, act_pp, toks, kd), BF16),
                (pltpu.VMEM((n_sec, act_pp, toks, kd), BF16),) * CHUNKS,
                pltpu.VMEM((n_dp, blk_pp, brows, d + LANES), BF16),
                pltpu.VMEM((n_dp, blk_pp, brows, d + LANES), BF16),
                pltpu.VMEM((CHUNKS, 2, chips, toks, kd + LANES), BF16),
                pltpu.VMEM((chips, toks, 2 * hd), F32),
                pltpu.VMEM((2, chips, toks, 2 * hd), F32),
                pltpu.VMEM((CHUNKS, chips, toks, kd), F32),
                pltpu.VMEM((CHUNKS, 2 * far, toks, kd), BF16),
                pltpu.VMEM((CHUNKS, 2 * far, toks, kd), BF16),
                dma((11,)),
                dma((n_sec - 1,)),
                dma((n_sec - 1, CHUNKS)),
                dma((2,)),
                dma((2,)),
                dma((2,)),
                dma((2,)),
                dma((CHUNKS,)),
                dma((2, far, CHUNKS)),
                dma((3, CHUNKS)),
                dma((CHUNKS,)),
                dma((2, far, CHUNKS)),
            ],
            compiler_params=pltpu.CompilerParams(
                collective_id=0, has_side_effects=True, vmem_limit_bytes=VMEM_BYTES - 2**16 - out_bytes
            ),
        )(section_sources, block_sources, loss_terms, activations, accumulators,
          pre_gain, query_weight, keyval_weight, output_weight, post_gain, rot)
        return pl.pallas_call(
            write_out,
            out_shape=(
                jax.ShapeDtypeStruct(activations.shape, BF16),
                jax.ShapeDtypeStruct(accumulators.shape, F32),
                jax.ShapeDtypeStruct((1, toks, d), BF16),
            ),
            in_specs=[vmem] * 3,
            out_specs=(in_hbm,) * 3,
            scratch_shapes=[dma((3,))],
            compiler_params=pltpu.CompilerParams(vmem_limit_bytes=4 * 2**20),
        )(*held)

    return on_device


def solution(mesh):
    placed = (
        P("section", "dp", None),
        P(),
        P("dp", "section", None),
        P(),
        P("section", "dp"),
        P("section", None),
        P("section", None, "dp"),
        P("section", None, "dp"),
        P("section", "dp", None),
        P("section", None),
    )
    return jax.shard_map(
        make_on_device(mesh.shape["section"], mesh.shape["dp"]),
        mesh=mesh,
        in_specs=placed,
        out_specs=(P("section", "dp", None), P("dp", "section", None), P("section", "dp", None)),
        check_vma=False,
    )
```

```python
import functools

import jax
import jax.numpy as jnp
import numpy as np
from jax import lax
from jax.experimental import pallas as pl
from jax.experimental.pallas import tpu as pltpu
from jax.sharding import PartitionSpec as P

LANES = 128
VMEM_BYTES = 67043328
CHUNKS = 6
MIXED = (0, 3, 1, 4, 2, 5)
AHEAD = ((0, 1, 3, 2, 4, 5), (3, 0, 4, 1, 5, 2))
SORTED = ((0, 1, 2, 3, 4, 5), (3, 4, 5, 0, 1, 2))
F32 = jnp.float32
BF16 = jnp.bfloat16


def pick(table, own, groups, per_group, peer, rank):
    def visit(j, carry):
        seen, found = carry
        source = table[peer * per_group + j]
        mine = (source // per_group == own).astype(jnp.int32)
        hit = mine * (seen == rank).astype(jnp.int32)
        return seen + mine, found + hit * (source % per_group)

    zero = jnp.int32(0)
    return lax.fori_loop(0, per_group, visit, (zero, zero), unroll=True)[1]


def origin(table, own, per_group, per_peer, entry):
    owner = table[own * per_group + entry] // per_group
    if per_peer == 1:
        return owner, 0

    def visit(j, seen):
        same = table[own * per_group + j] // per_group == owner
        return seen + same.astype(jnp.int32) * (j < entry).astype(jnp.int32)

    return owner, lax.fori_loop(0, per_group, visit, jnp.int32(0))


def rotary_tables(length, width):
    half = width // 2
    freqs = np.float32(10000.0) ** (np.float32(-2.0) * np.arange(half, dtype=np.float32) / np.float32(width))
    angles = np.arange(length, dtype=np.float32)[:, None] * freqs.astype(np.float32)[None, :]
    cosine, sine = np.cos(angles.astype(np.float64)), np.sin(angles.astype(np.float64))
    return np.stack(
        [np.concatenate([cosine, cosine], 1), np.concatenate([-sine, sine], 1)]
    ).astype(np.float32)


def kernel(
    dims,
    secs_hbm, blks_hbm, loss_hbm, act_hbm, acc_hbm, pre_hbm, wq_hbm, wkv_hbm, wo_hbm, post_hbm, rot_hbm,
    moved, accout, outbuf,
    secs, blks, loss, act, acc, pre, post, rot, turn, w, wo,
    stage, actrecv, sacc, racc,
    gath, qs, kvs, part, ring_in, ring_out,
    load_sem, act_out, act_sem, w_sem, wq_sem, wo_sem, blk_sem, ag_out, ag_sem, fwd_sem, ring_done, ring_sem,
):
    n_sec, n_dp = dims
    mb, toks, d = act.shape
    blk, brows, _ = acc.shape
    act_pp, blk_pp = mb // n_sec, blk // n_dp
    chips = n_dp // 2
    far = chips // 2
    kd = d // CHUNKS
    length = n_dp * toks
    hd = wq_hbm.shape[2]
    sec, me = lax.axis_index("section"), lax.axis_index("dp")
    core, chip = me % 2, me // 2
    side, rung = chip % 2, chip // 2
    pos = rung * (1 - side) + (chips - 1 - rung) * side

    def chip_at(p):
        q = (p + 2 * chips) % chips
        s = q // (chips // 2)
        return 2 * (q * (1 - s) + (chips - 1 - q) * s) + s

    def device(p):
        return {"dp": 2 * chip_at(p) + core}

    partner = {"dp": me + 1 - 2 * core}
    mate = {"dp": 2 * (2 * rung + 1 - side) + core}
    cross = far // 2
    from_middle = ((pos == cross) | (pos == chips - cross), (pos == cross - 1) | (pos == chips - cross - 1))

    def remote(src, dst, send_sem, recv_sem, dev):
        return pltpu.make_async_remote_copy(
            src_ref=src, dst_ref=dst, send_sem=send_sem, recv_sem=recv_sem,
            device_id=dev, device_id_type=pl.DeviceIdType.MESH,
        )

    barrier = pltpu.get_barrier_semaphore()
    for o in range(1, n_sec):
        pl.semaphore_signal(barrier, inc=1, device_id={"section": (sec + o) % n_sec},
                            device_id_type=pl.DeviceIdType.MESH)
    for near in (device(pos + 1), device(pos - 1), partner, mate):
        pl.semaphore_signal(barrier, inc=1, device_id=near, device_id_type=pl.DeviceIdType.MESH)

    kv_cols = pl.ds(pl.multiple_of(2 * hd + core * hd, LANES), hd)
    q_cols = pl.ds(pl.multiple_of(core * hd, LANES), hd)
    wo_rows = pl.ds(pl.multiple_of(core * hd, LANES), hd)
    names = ("secs", "act", "pre", "wkv", "wo", "blks", "loss", "acc", "wq", "rot", "post")
    pairs = [
        (secs_hbm, secs), (act_hbm, act), (pre_hbm, pre), (wkv_hbm.at[0], w.at[:, kv_cols]),
        (wo_hbm.at[0], wo.at[wo_rows]), (blks_hbm, blks), (loss_hbm, loss), (acc_hbm, acc),
        (wq_hbm.at[0], w.at[:, q_cols]), (rot_hbm, rot), (post_hbm, post),
    ]
    loads = {
        name: pltpu.make_async_copy(src, dst, load_sem.at[i])
        for i, (name, (src, dst)) in enumerate(zip(names, pairs))
    }
    for name in names:
        loads[name].start()

    loads["secs"].wait()
    loads["act"].wait()
    for q in range(n_sec):
        for r in range(act_pp):
            block = act[pick(secs, sec, n_sec, mb, q, r)]
            for k in range(CHUNKS):
                stage[q, k, r] = block[:, k * kd:(k + 1) * kd]
    pl.semaphore_wait(barrier, n_sec - 1 + 4)
    act_copies = [[] for _ in range(CHUNKS)]
    for k in MIXED:
        for o in range(1, n_sec):
            q = (sec + o) % n_sec
            copy = remote(stage.at[q, k], actrecv[k].at[sec], act_out.at[o - 1], act_sem.at[o - 1, k], {"section": q})
            copy.start()
            act_copies[k].append(copy)
    for k in range(CHUNKS):
        actrecv[k][sec] = stage[sec, k]

    loads["wkv"].wait()
    loads["wo"].wait()
    loads["wq"].wait()

    def whole(ref, sems):
        return remote(ref, ref, sems.at[0], sems.at[1], partner)

    kv_copy, q_copy = whole(w.at[:, kv_cols], w_sem), whole(w.at[:, q_cols], wq_sem)
    wo_copy = whole(wo.at[wo_rows], wo_sem)

    def share(ref, sems):
        remote(ref, ref, sems.at[0], sems.at[1], partner).start()

    for name in ("acc", "blks", "loss"):
        loads[name].wait()
    term = jnp.full((brows, LANES), loss[0, 0], F32)
    high = term.astype(BF16).astype(F32)
    lane = lax.broadcasted_iota(jnp.int32, (brows, LANES), 1)
    row = lax.broadcasted_iota(jnp.int32, (brows, LANES), 0)
    tail = jnp.where(row > 0, 0.0, jnp.where(lane == 0, high, jnp.where(lane == 1, term - high, 0.0)))

    def pack(p, carry):
        for r in range(blk_pp):
            sacc[p, r, :, pl.ds(0, d)] = acc[pick(blks, me, n_dp, blk, p, r)].astype(BF16)
            sacc[p, r, :, pl.ds(d, LANES)] = tail.astype(BF16)
        return carry

    lax.fori_loop(0, n_dp // 2, pack, 0)
    loads["pre"].wait()

    def hops(way, k):
        return far if (k < CHUNKS // 2) == (way == 0) else far - 1

    step_of = (1, -1)

    def width(k):
        return kd + LANES if k == MIXED[-1] else kd

    def slot(way, hop):
        return 0 if hop == 0 else min(2 * hop - 1 + way, chips - 1)

    def blocks_of(k, c, slots):
        return gath.at[k, c, slots, :, pl.ds(0, width(k))]

    def gather_copy(way, hop, k):
        return remote(blocks_of(k, core, slot(way, hop - 1)), blocks_of(k, core, slot(way, hop)),
                      ag_out.at[k], ag_sem.at[way, hop - 1, k], device(pos + step_of[way]))

    def forward(way, hop, k):
        if hop < hops(way, k):
            if hop < cross:
                gather_copy(way, hop + 1, k).start()
            else:
                pl.when(jnp.logical_not(from_middle[1 - way]))(gather_copy(way, hop + 1, k).start)
        there = far + 1 - hop
        if cross < there <= hops(1 - way, k):
            across = remote(blocks_of(k, core, slot(way, hop)), blocks_of(k, core, slot(1 - way, there)),
                            ag_out.at[k], ag_sem.at[1 - way, there - 1, k], mate)
            pl.when(from_middle[way])(across.start)

    near = 2 * (far - 2) + 1
    spans = (slice(0, near), slice(near, chips))

    def pass_on(j, k):
        block = blocks_of(k, core, j)
        remote(block, block, fwd_sem.at[0, k], fwd_sem.at[1 if j < near else 2, k], partner).start()

    square = jnp.zeros((toks, 1), F32)
    for k in MIXED:
        for copy in act_copies[k]:
            copy.wait_recv()
        owner, number = origin(secs, sec, mb, act_pp, 0)
        piece = actrecv[k][owner, number].astype(F32)
        square = square + jnp.sum(piece * piece, axis=-1, keepdims=True)
        gath[k, core, 0, :, pl.ds(0, kd)] = (piece * pre[:, k * kd:(k + 1) * kd]).astype(BF16)
        if k == MIXED[-1]:
            root = jnp.broadcast_to(lax.rsqrt(square / d + 1e-06), (toks, LANES))
            high = root.astype(BF16).astype(F32)
            lane = lax.broadcasted_iota(jnp.int32, (toks, LANES), 1)
            gath[k, core, 0, :, pl.ds(kd, LANES)] = jnp.where(
                lane == 0, high, jnp.where(lane == 1, root - high, 0.0)).astype(BF16)
        for way in range(2):
            gather_copy(way, 1, k).start()
        pass_on(0, k)

    other = me + 1 - 2 * core

    def project(k, part_of, fresh):
        span = spans[part_of]
        count = span.stop - span.start

        def add(ref, index, rows, cols):
            rows = rows.reshape(-1, kd)
            terms = jnp.dot(rows, w[k * kd:(k + 1) * kd, cols], preferred_element_type=F32)
            terms = terms.reshape(ref[index].shape)
            ref[index] = terms if fresh else ref[index] + terms

        add(qs, span, gath[k, core, span, :, pl.ds(0, kd)], slice(0, 2 * hd))
        block = blocks_of(k, 1 - core, pl.ds(span.start, count))
        remote(block, block, fwd_sem.at[0, k], fwd_sem.at[1 + part_of, k], partner).wait_recv()
        add(kvs, (slice(None), span), gath[k, :, span, :, pl.ds(0, kd)], slice(2 * hd, 4 * hd))

    def send_block(peer):
        remote(sacc.at[peer], racc.at[me], blk_sem.at[0], blk_sem.at[1], {"dp": peer}).start()

    def send_blocks(places):
        for way, hop in places:
            for c in range(2):
                send_block(2 * chip_at(pos + step_of[way] * hop) + (core + c) % 2)

    loads["rot"].wait()
    for j in range(chips):
        place = chip_at(pos + (j + 1) // 2 * (1 - 2 * (j % 2)))
        for c in range(2):
            for t in range(2):
                turn[t, c, j] = rot[t, place, c]

    half = CHUNKS // 2
    quarter = n_dp // 8
    for hop in range(1, far + 1):
        order = (MIXED, MIXED) if hop == 1 else AHEAD if hop < far else SORTED
        for i in range(CHUNKS if hop < far else half):
            for way in range(2):
                k = order[way][i]
                gather_copy(way, hop, k).wait_recv()
                forward(way, hop, k)
                pass_on(slot(way, hop), k)
            if hop == 1:
                rows = pl.ds(i * kd, kd)
                share(w.at[rows, kv_cols], w_sem)
                share(w.at[rows, q_cols], wq_sem)
                if i < 4:
                    lax.fori_loop((4 + i) * quarter, (5 + i) * quarter, pack, 0)
                elif i == 4:
                    racc[me] = sacc[me]
                    send_block(other)
            if hop == 2:
                share(wo.at[wo_rows, pl.ds(i * kd, kd)], wo_sem)
            if hop == far - 1 and i == CHUNKS - 1:
                send_blocks([(way, far - h) for h in range(1, far) for way in range(2)])
            if hop == far - 1 and i == 1:
                kv_copy.wait_recv()
                q_copy.wait_recv()
            if hop == far - 1 and i > 0:
                project(i - 1, 0, i == 1)
            if hop == far and i > 0:
                project(i - 1, 1, i == 1)
                project(half + i - 1, 1, False)
            if hop == far and i == 0:
                send_blocks([(0, far)])
        if hop == far - 1:
            project(CHUNKS - 1, 0, False)
    project(half - 1, 1, False)
    project(CHUNKS - 1, 1, False)

    def root_of(parts):
        return jnp.sum(parts.reshape(-1, LANES).astype(F32), axis=-1, keepdims=True)

    def turned(v, tables, root):
        return (v * (tables[0].reshape(-1, hd) * root) + pltpu.roll(v, hd // 2, 1) * (tables[1].reshape(-1, hd) * root)).astype(BF16)

    mine = chips * toks
    root = root_of(gath[CHUNKS - 1, :, :, :, pl.ds(kd, LANES)])
    own_root = root_of(gath[CHUNKS - 1, core, :, :, pl.ds(kd, LANES)])
    own_turn = turn[0, core], turn[1, core]

    def token_at(row, first_core):
        block = row // toks
        j = block % chips
        p = (pos + (j + 1) // 2 * (1 - 2 * (j % 2)) + 2 * chips) % chips
        s = p // (chips // 2)
        return (2 * (2 * (p * (1 - s) + (chips - 1 - p) * s) + s) + first_core + block // chips) * toks + row % toks

    q_rows = qs[...].reshape(mine, 2 * hd)
    kv_rows = kvs[...].reshape(length, 2 * hd)
    queries = jnp.concatenate([turned(q_rows[:, 0:hd], own_turn, own_root), turned(q_rows[:, hd:2 * hd], own_turn, own_root)], axis=0)
    keys = turned(kv_rows[:, 0:hd], (turn[0], turn[1]), root)
    values = (kv_rows[:, hd:2 * hd] * root).astype(BF16)
    scores = lax.dot_general(queries, keys, (((1,), (1,)), ((), ())), preferred_element_type=F32)
    scores = scores * ((d / n_dp) ** (-0.5) / 50.0)
    query_token = token_at(lax.broadcasted_iota(jnp.int32, (2 * mine, 1), 0) % mine, core)
    key_token = token_at(lax.broadcasted_iota(jnp.int32, (1, length), 1), 0)
    expd = jnp.where(key_token <= query_token, jnp.exp(50.0 * jnp.tanh(scores)), 0.0)
    denominator = jnp.sum(expd, axis=-1, keepdims=True)
    numer = jnp.dot(expd.astype(BF16), values, preferred_element_type=F32)
    attended = (numer / denominator).astype(BF16)
    both = jnp.concatenate([attended[0:mine], attended[mine:2 * mine]], axis=1)
    wo_copy.wait_recv()

    def ring_copy(way, step, k):
        goal = device(pos + step_of[way])
        if hops(way, k) - step + 1 > cross:
            goal = {"dp": jnp.where(from_middle[1 - way], mate["dp"], goal["dp"])}
        return remote(ring_out.at[k, way * far + step - 1], ring_in.at[k, way * far + step - 1],
                      ring_done.at[k], ring_sem.at[way, step - 1, k], goal)

    def launch(way, step, k, total):
        ring_out[k, way * far + step - 1] = total.astype(BF16)
        ring_copy(way, step, k).start()

    for k in MIXED:
        terms = jnp.dot(both, wo[:, k * kd:(k + 1) * kd], preferred_element_type=F32)
        part[k] = terms.reshape(chips, toks, kd)
        way = 0 if hops(0, k) == far else 1
        launch(way, 1, k, part[k, chips - 1])
    for j in range(half):
        for way in range(2):
            k = SORTED[way][half + j]
            launch(way, 1, k, part[k, slot(1 - way, hops(way, k))])
    for j in range(mb):
        owner, number = origin(secs, sec, mb, act_pp, j)
        for k in range(CHUNKS):
            moved[j, :, k * kd:(k + 1) * kd] = actrecv[k][owner, number]

    waited, early = set(), set()

    def take(way, step, k):
        copy = ring_copy(way, step, k)
        if (way, step, k) in early:
            pl.when(jnp.logical_not(from_middle[way]))(copy.wait_recv)
        else:
            copy.wait_recv()
        waited.add((way, step, k))
        return ring_in[k, way * far + step - 1].astype(F32)

    def relay(way, step, k):
        left = hops(way, k) - step
        came = take(way, step, k)
        if left + 1 > cross:
            came = jnp.where(from_middle[way], 0.0, came)
        target = slot(1 - way, left)
        there = far + 1 - left
        if cross < there <= hops(1 - way, k):
            other_step = hops(1 - way, k) - there + 1
            late = (1 - way, other_step, k) not in waited
            if late:
                early.add((1 - way, other_step, k))

            @pl.when(from_middle[1 - way])
            def _():
                if late:
                    ring_copy(1 - way, other_step, k).wait_recv()
                part[k, target] = part[k, target] + ring_in[k, (1 - way) * far + other_step - 1].astype(F32)

        launch(way, step + 1, k, part[k, target] + came)

    for step in range(1, far):
        for group in range(2):
            for j in range(half):
                for way in range(2):
                    k = SORTED[way][group * half + j]
                    if step < hops(way, k):
                        relay(way, step, k)

    others = pl.ds(0, n_dp - 1)
    all_blocks = remote(sacc.at[others], racc.at[others], blk_sem.at[0], blk_sem.at[1], partner)
    all_blocks.wait_recv()
    scale_sum = jnp.sum(racc[:, 0, :, pl.ds(d, LANES)].astype(F32), axis=0)
    factor = n_dp / jnp.sum(jnp.sum(scale_sum, axis=0, keepdims=True), axis=1, keepdims=True)

    def unpack(b, carry):
        owner, number = origin(blks, me, blk, blk_pp, b)
        accout[b] = racc[owner, number, :, pl.ds(0, d)].astype(F32) * factor
        return carry

    lax.fori_loop(0, blk, unpack, 0)

    pieces = []
    for k in range(CHUNKS):
        total = part[k, 0]
        for way in range(2):
            total = total + take(way, hops(way, k), k)
        pieces.append(total)
    loads["post"].wait()
    square = sum(jnp.sum(t * t, axis=-1, keepdims=True) for t in pieces)
    scale = lax.rsqrt(square / d + 1e-06)
    for k in range(CHUNKS):
        cols = slice(k * kd, (k + 1) * kd)
        outbuf[0, :, cols] = (
            moved[0, :, cols].astype(F32) + pieces[k] * scale * post[:, cols]
        ).astype(BF16)
    for copy in (kv_copy, q_copy, wo_copy, all_blocks):
        copy.wait_send()
    for o in range(1, n_sec):
        q = (sec + o) % n_sec
        remote(stage.at[q], stage.at[q], act_out.at[o - 1], act_sem.at[o - 1, 0], {"section": q}).wait_send()
    for k in range(CHUNKS):
        for places, sem in ((slice(None), fwd_sem.at[0, k]), (pl.ds(0, chips - 1), ag_out.at[k])):
            block = blocks_of(k, core, places)
            remote(block, block, sem, fwd_sem.at[1, k], partner).wait_send()
        block = ring_out.at[k, pl.ds(0, chips - 1)]
        remote(block, block, ring_done.at[k], fwd_sem.at[1, k], partner).wait_send()


def write_out(moved, accout, outbuf, moved_hbm, newacc_hbm, check_hbm, sems):
    copies = [
        pltpu.make_async_copy(src, dst, sems.at[i])
        for i, (src, dst) in enumerate([(accout, newacc_hbm), (moved, moved_hbm), (outbuf, check_hbm)])
    ]
    for copy in copies:
        copy.start()
    for copy in copies:
        copy.wait()


def make_on_device(n_sec, n_dp):
    def on_device(activations, section_sources, accumulators, block_sources, loss_terms,
                  pre_gain, query_weight, keyval_weight, output_weight, post_gain):
        mb, toks, d = activations.shape
        blk, brows, _ = accumulators.shape
        hd = query_weight.shape[2]
        chips, far, kd, length = n_dp // 2, n_dp // 4, d // CHUNKS, n_dp * toks
        rot = jnp.asarray(rotary_tables(length, hd).reshape(2, chips, 2, toks, hd))
        smem = pltpu.SMEM
        in_hbm = pl.BlockSpec(memory_space=pltpu.HBM)
        vmem = pl.BlockSpec(memory_space=pltpu.VMEM)
        dma = pltpu.SemaphoreType.DMA
        act_pp, blk_pp = mb // n_sec, blk // n_dp
        out_bytes = activations.size * 2 + accumulators.size * 4 + toks * d * 2
        held = pl.pallas_call(
            functools.partial(kernel, (n_sec, n_dp)),
            out_shape=(
                pltpu.VMEM(activations.shape, BF16),
                pltpu.VMEM(accumulators.shape, F32),
                pltpu.VMEM((1, toks, d), BF16),
            ),
            in_specs=[in_hbm] * 11,
            out_specs=(vmem,) * 3,
            scratch_shapes=[
                smem(section_sources.shape, jnp.int32),
                smem(block_sources.shape, jnp.int32),
                smem((1, 1), F32),
                pltpu.VMEM(activations.shape, BF16),
                pltpu.VMEM(accumulators.shape, F32),
                pltpu.VMEM((1, d), F32),
                pltpu.VMEM((1, d), F32),
                pltpu.VMEM(rot.shape, F32),
                pltpu.VMEM((2, 2, chips, toks, hd), F32),
                pltpu.VMEM((d, 4 * hd), BF16),
                pltpu.VMEM((2 * hd, d), BF16),
                pltpu.VMEM((n_sec, CHUNKS, act_pp, toks, kd), BF16),
                (pltpu.VMEM((n_sec, act_pp, toks, kd), BF16),) * CHUNKS,
                pltpu.VMEM((n_dp, blk_pp, brows, d + LANES), BF16),
                pltpu.VMEM((n_dp, blk_pp, brows, d + LANES), BF16),
                pltpu.VMEM((CHUNKS, 2, chips, toks, kd + LANES), BF16),
                pltpu.VMEM((chips, toks, 2 * hd), F32),
                pltpu.VMEM((2, chips, toks, 2 * hd), F32),
                pltpu.VMEM((CHUNKS, chips, toks, kd), F32),
                pltpu.VMEM((CHUNKS, 2 * far, toks, kd), BF16),
                pltpu.VMEM((CHUNKS, 2 * far, toks, kd), BF16),
                dma((11,)),
                dma((n_sec - 1,)),
                dma((n_sec - 1, CHUNKS)),
                dma((2,)),
                dma((2,)),
                dma((2,)),
                dma((2,)),
                dma((CHUNKS,)),
                dma((2, far, CHUNKS)),
                dma((3, CHUNKS)),
                dma((CHUNKS,)),
                dma((2, far, CHUNKS)),
            ],
            compiler_params=pltpu.CompilerParams(
                collective_id=0, has_side_effects=True, vmem_limit_bytes=VMEM_BYTES - 2**16 - out_bytes
            ),
        )(section_sources, block_sources, loss_terms, activations, accumulators,
          pre_gain, query_weight, keyval_weight, output_weight, post_gain, rot)
        return pl.pallas_call(
            write_out,
            out_shape=(
                jax.ShapeDtypeStruct(activations.shape, BF16),
                jax.ShapeDtypeStruct(accumulators.shape, F32),
                jax.ShapeDtypeStruct((1, toks, d), BF16),
            ),
            in_specs=[vmem] * 3,
            out_specs=(in_hbm,) * 3,
            scratch_shapes=[dma((3,))],
            compiler_params=pltpu.CompilerParams(vmem_limit_bytes=4 * 2**20),
        )(*held)

    return on_device


def solution(mesh):
    placed = (
        P("section", "dp", None),
        P(),
        P("dp", "section", None),
        P(),
        P("section", "dp"),
        P("section", None),
        P("section", None, "dp"),
        P("section", None, "dp"),
        P("section", "dp", None),
        P("section", None),
    )
    return jax.shard_map(
        make_on_device(mesh.shape["section"], mesh.shape["dp"]),
        mesh=mesh,
        in_specs=placed,
        out_specs=(P("section", "dp", None), P("dp", "section", None), P("section", "dp", None)),
        check_vma=False,
    )
```

```python
import functools

import jax
import jax.numpy as jnp
import numpy as np
from jax import lax
from jax.experimental import pallas as pl
from jax.experimental.pallas import tpu as pltpu
from jax.sharding import PartitionSpec as P

LANES = 128
VMEM_BYTES = 67043328
CHUNKS = 6
MIXED = (0, 3, 1, 4, 2, 5)
AHEAD = ((0, 1, 3, 2, 4, 5), (3, 0, 4, 1, 5, 2))
SORTED = ((0, 1, 2, 3, 4, 5), (3, 4, 5, 0, 1, 2))
F32 = jnp.float32
BF16 = jnp.bfloat16


def pick(table, own, groups, per_group, peer, rank):
    def visit(j, carry):
        seen, found = carry
        source = table[peer * per_group + j]
        mine = (source // per_group == own).astype(jnp.int32)
        hit = mine * (seen == rank).astype(jnp.int32)
        return seen + mine, found + hit * (source % per_group)

    zero = jnp.int32(0)
    return lax.fori_loop(0, per_group, visit, (zero, zero), unroll=True)[1]


def origin(table, own, per_group, per_peer, entry):
    owner = table[own * per_group + entry] // per_group
    if per_peer == 1:
        return owner, 0

    def visit(j, seen):
        same = table[own * per_group + j] // per_group == owner
        return seen + same.astype(jnp.int32) * (j < entry).astype(jnp.int32)

    return owner, lax.fori_loop(0, per_group, visit, jnp.int32(0))


def rotary_tables(length, width):
    half = width // 2
    freqs = np.float32(10000.0) ** (np.float32(-2.0) * np.arange(half, dtype=np.float32) / np.float32(width))
    angles = np.arange(length, dtype=np.float32)[:, None] * freqs.astype(np.float32)[None, :]
    cosine, sine = np.cos(angles.astype(np.float64)), np.sin(angles.astype(np.float64))
    return np.stack(
        [np.concatenate([cosine, cosine], 1), np.concatenate([-sine, sine], 1)]
    ).astype(np.float32)


def kernel(
    dims,
    secs_hbm, blks_hbm, loss_hbm, act_hbm, acc_hbm, pre_hbm, wq_hbm, wkv_hbm, wo_hbm, post_hbm, rot_hbm,
    moved, accout, outbuf,
    secs, blks, loss, act, acc, pre, post, rot, turn, seen, w, wo,
    stage, actrecv, sacc, racc,
    gath, qs, kvs, part, ring_in, ring_out,
    ready, load_sem, act_out, act_sem, w_sem, blk_sem, ag_out, ag_sem, fwd_out, fwd_sem, ring_done, ring_sem,
):
    n_sec, n_dp = dims
    mb, toks, d = act.shape
    blk, brows, _ = acc.shape
    act_pp, blk_pp = mb // n_sec, blk // n_dp
    chips = n_dp // 2
    far = chips // 2
    kd = d // CHUNKS
    length = n_dp * toks
    hd = wq_hbm.shape[2]
    sec, me = lax.axis_index("section"), lax.axis_index("dp")
    core, chip = me % 2, me // 2
    side, rung = chip % 2, chip // 2
    pos = rung * (1 - side) + (chips - 1 - rung) * side

    def chip_at(p):
        q = (p + 2 * chips) % chips
        s = q // (chips // 2)
        return 2 * (q * (1 - s) + (chips - 1 - q) * s) + s

    def device(p):
        return {"dp": 2 * chip_at(p) + 1 - core}

    partner = {"dp": me + 1 - 2 * core}
    mate = {"dp": 2 * (2 * rung + 1 - side) + 1 - core}
    cross = far // 2
    from_middle = ((pos == cross) | (pos == chips - cross), (pos == cross - 1) | (pos == chips - cross - 1))

    def remote(src, dst, send_sem, recv_sem, dev):
        return pltpu.make_async_remote_copy(
            src_ref=src, dst_ref=dst, send_sem=send_sem, recv_sem=recv_sem,
            device_id=dev, device_id_type=pl.DeviceIdType.MESH,
        )

    barrier = pltpu.get_barrier_semaphore()
    for o in range(1, n_sec):
        pl.semaphore_signal(barrier, inc=1, device_id={"section": (sec + o) % n_sec},
                            device_id_type=pl.DeviceIdType.MESH)
    def same(dev):
        return {"dp": dev["dp"] + 2 * core - 1}

    for near in (same(device(pos + 1)), same(device(pos - 1)), partner, same(mate)):
        pl.semaphore_signal(barrier, inc=1, device_id=near, device_id_type=pl.DeviceIdType.MESH)

    kv_cols = pl.ds(pl.multiple_of(2 * hd + core * hd, LANES), hd)
    q_cols = pl.ds(pl.multiple_of(core * hd, LANES), hd)
    wo_rows = pl.ds(pl.multiple_of(core * hd, LANES), hd)
    names = ("secs", "act", "pre", "wkv", "blks", "loss", "acc", "rot", "post", "wo", "wq")
    pairs = [
        (secs_hbm, secs), (act_hbm, act), (pre_hbm, pre), (wkv_hbm.at[0], w.at[:, kv_cols]),
        (blks_hbm, blks), (loss_hbm, loss), (acc_hbm, acc), (rot_hbm, rot), (post_hbm, post),
        (wo_hbm.at[0], wo.at[wo_rows]), (wq_hbm.at[0], w.at[:, q_cols]),
    ]
    loads = {
        name: pltpu.make_async_copy(src, dst, load_sem.at[names.index("wkv") if name in ("wq", "wo") else i])
        for i, (name, (src, dst)) in enumerate(zip(names, pairs))
    }
    for name in ("secs", "act", "wkv", "wq", "wo", "pre", "blks", "loss", "acc", "rot", "post"):
        loads[name].start()

    loads["secs"].wait()
    loads["act"].wait()
    for q in range(n_sec):
        for r in range(act_pp):
            block = act[pick(secs, sec, n_sec, mb, q, r)]
            for k in range(CHUNKS):
                stage[q, k, r] = block[:, k * kd:(k + 1) * kd]
    pl.semaphore_wait(barrier, n_sec - 1 + 4)
    pl.semaphore_signal(ready, inc=1, device_id=partner, device_id_type=pl.DeviceIdType.MESH)
    act_copies = [[] for _ in range(CHUNKS)]
    for k in MIXED:
        for o in range(1, n_sec):
            q = (sec + o) % n_sec
            copy = remote(stage.at[q, k], actrecv[k].at[sec], act_out.at[o - 1], act_sem.at[o - 1, k], {"section": q})
            copy.start()
            act_copies[k].append(copy)
    for k in range(CHUNKS):
        actrecv[k][sec] = stage[sec, k]

    mine = chips * toks

    def token_at(row, first_core):
        block = row // toks
        j = block % chips
        p = (pos + (j + 1) // 2 * (1 - 2 * (j % 2)) + 2 * chips) % chips
        s = p // (chips // 2)
        return (2 * (2 * (p * (1 - s) + (chips - 1 - p) * s) + s) + (first_core + block // chips + (j + 1) // 2) % 2) * toks + row % toks

    query_token = token_at(lax.broadcasted_iota(jnp.int32, (2 * mine, 1), 0) % mine, core)
    key_token = token_at(lax.broadcasted_iota(jnp.int32, (1, length), 1), 0)
    seen[...] = (key_token <= query_token).astype(F32)

    three = w.at[:, pl.ds(0, 3 * hd)]
    weights_loaded = load_sem.at[names.index("wkv")]
    remote(three, three, weights_loaded, weights_loaded, partner).wait_recv()
    two = w.at[:, pl.ds(0, 2 * hd)]
    weights = remote(two, two, w_sem.at[0], w_sem.at[1], partner)
    wo_copy = remote(wo.at[wo_rows], wo.at[wo_rows], w_sem.at[2], w_sem.at[3], partner)

    def share(ref, i):
        remote(ref, ref, w_sem.at[i], w_sem.at[i + 1], partner).start()

    for name in ("acc", "blks", "loss"):
        loads[name].wait()
    term = jnp.full((brows, LANES), loss[0, 0], F32)
    high = term.astype(BF16).astype(F32)
    lane = lax.broadcasted_iota(jnp.int32, (brows, LANES), 1)
    row = lax.broadcasted_iota(jnp.int32, (brows, LANES), 0)
    tail = jnp.where(row > 0, 0.0, jnp.where(lane == 0, high, jnp.where(lane == 1, term - high, 0.0)))

    def pack(p, carry):
        for r in range(blk_pp):
            sacc[p, r, :, pl.ds(0, d)] = acc[pick(blks, me, n_dp, blk, p, r)].astype(BF16)
            sacc[p, r, :, pl.ds(d, LANES)] = tail.astype(BF16)
        return carry

    lax.fori_loop(0, n_dp // 2, pack, 0)
    loads["pre"].wait()

    def hops(way, k):
        return far if (k < CHUNKS // 2) == (way == 0) else far - 1

    step_of = (1, -1)

    def width(k):
        return kd + LANES if k == MIXED[-1] else kd

    def place_of(way, hop, k):
        return (hop - 1) * 2 * CHUNKS + (way * CHUNKS if hop < far else 0) + k

    def last(k):
        return 1 if k == MIXED[-1] else 0

    def slot(way, hop):
        return 0 if hop == 0 else min(2 * hop - 1 + way, chips - 1)

    def blocks_of(k, c, slots):
        return gath.at[k, c, slots, :, pl.ds(0, width(k))]

    def gather_copy(way, hop, k):
        return remote(blocks_of(k, core, slot(way, hop - 1)), blocks_of(k, 1 - core, slot(way, hop)),
                      ag_out.at[last(k)], ag_sem.at[place_of(way, hop, k)], device(pos + step_of[way]))

    def forward(way, hop, k):
        if hop < hops(way, k):
            if hop < cross:
                gather_copy(way, hop + 1, k).start()
            else:
                pl.when(jnp.logical_not(from_middle[1 - way]))(gather_copy(way, hop + 1, k).start)
        there = far + 1 - hop
        if cross < there <= hops(1 - way, k):
            across = remote(blocks_of(k, core, slot(way, hop)), blocks_of(k, 1 - core, slot(1 - way, there)),
                            ag_out.at[last(k)], ag_sem.at[place_of(1 - way, there, k)], mate)
            pl.when(from_middle[way])(across.start)

    near = 2 * (far - 2) + 1
    spans = (slice(0, near), slice(near, chips))

    def pass_on(j, k):
        block = blocks_of(k, core, j)
        remote(block, block, fwd_out.at[last(k)], fwd_sem.at[0 if j < near else 1, k], partner).start()

    pl.semaphore_wait(ready, 1)
    square = jnp.zeros((toks, 1), F32)
    for k in MIXED:
        for copy in act_copies[k]:
            copy.wait_recv()
        owner, number = origin(secs, sec, mb, act_pp, 0)
        piece = actrecv[k][owner, number].astype(F32)
        square = square + jnp.sum(piece * piece, axis=-1, keepdims=True)
        gath[k, core, 0, :, pl.ds(0, kd)] = (piece * pre[:, k * kd:(k + 1) * kd]).astype(BF16)
        if k == MIXED[-1]:
            root = jnp.broadcast_to(lax.rsqrt(square / d + 1e-06), (toks, LANES))
            high = root.astype(BF16).astype(F32)
            lane = lax.broadcasted_iota(jnp.int32, (toks, LANES), 1)
            gath[k, core, 0, :, pl.ds(kd, LANES)] = jnp.where(
                lane == 0, high, jnp.where(lane == 1, root - high, 0.0)).astype(BF16)
        for way in range(2):
            gather_copy(way, 1, k).start()
        pass_on(0, k)

    other = me + 1 - 2 * core

    def project(ks, part_of, fresh):
        span = spans[part_of]
        count = span.stop - span.start

        def add(ref, index, cores, cols):
            terms = sum(
                jnp.dot(gath[k, cores, span, :, pl.ds(0, kd)].reshape(-1, kd), w[k * kd:(k + 1) * kd, cols],
                        preferred_element_type=F32)
                for k in ks
            ).reshape(ref[index].shape)
            ref[index] = terms if fresh else ref[index] + terms

        add(qs, span, core, slice(0, 2 * hd))
        for k in ks:
            block = blocks_of(k, 1 - core, pl.ds(span.start, count))
            remote(block, block, fwd_out.at[0], fwd_sem.at[part_of, k], partner).wait_recv()
        add(kvs, (slice(None), span), slice(None), slice(2 * hd, 4 * hd))

    def send_block(peer):
        remote(sacc.at[peer], racc.at[me], blk_sem.at[0], blk_sem.at[1], {"dp": peer}).start()

    def send_blocks(places):
        for way, hop in places:
            for c in range(2):
                send_block(2 * chip_at(pos + step_of[way] * hop) + (core + c) % 2)

    loads["rot"].wait()
    for j in range(chips):
        place = chip_at(pos + (j + 1) // 2 * (1 - 2 * (j % 2)))
        for c in range(2):
            for t in range(2):
                turn[t, c, j] = rot[t, place, (c + (j + 1) // 2) % 2]

    half = CHUNKS // 2
    quarter = n_dp // 8
    for hop in range(1, far + 1):
        order = (MIXED, MIXED) if hop == 1 else AHEAD if hop < far else SORTED
        for i in range(CHUNKS if hop < far else half):
            for way in range(2):
                k = order[way][i]
                gather_copy(way, hop, k).wait_recv()
                forward(way, hop, k)
                pass_on(slot(way, hop), k)
            if hop == 1:
                rows = pl.ds(i * kd, kd)
                share(w.at[rows, kv_cols], 0)
                share(w.at[rows, q_cols], 0)
                if i < 4:
                    lax.fori_loop((4 + i) * quarter, (5 + i) * quarter, pack, 0)
                elif i == 4:
                    racc[me] = sacc[me]
                    send_block(other)
            if hop == 2:
                share(wo.at[wo_rows, pl.ds(i * kd, kd)], 2)
            if hop == far - 1 and i == CHUNKS - 1:
                send_blocks([(way, far - h) for h in range(1, far) for way in range(2)])
            if hop == far - 1 and i == 1:
                weights.wait_recv()
            if hop == far - 1 and i % 2 == 1:
                project(MIXED[i - 1:i + 1], 0, i == 1)
            if hop == far and i > 0:
                project((i - 1, half + i - 1), 1, i == 1)
            if hop == far and i == 0:
                send_blocks([(0, far)])
    project((half - 1, CHUNKS - 1), 1, False)

    def root_of(parts):
        return jnp.sum(parts.reshape(-1, LANES).astype(F32), axis=-1, keepdims=True)

    def turned(v, tables, root):
        return (v * (tables[0].reshape(-1, hd) * root) + pltpu.roll(v, hd // 2, 1) * (tables[1].reshape(-1, hd) * root)).astype(BF16)

    root = root_of(gath[CHUNKS - 1, :, :, :, pl.ds(kd, LANES)])
    own_root = root_of(gath[CHUNKS - 1, core, :, :, pl.ds(kd, LANES)])
    own_turn = turn[0, core], turn[1, core]

    q_rows = qs[...].reshape(mine, 2 * hd)
    kv_rows = kvs[...].reshape(length, 2 * hd)
    queries = jnp.concatenate([turned(q_rows[:, 0:hd], own_turn, own_root), turned(q_rows[:, hd:2 * hd], own_turn, own_root)], axis=0)
    keys = turned(kv_rows[:, 0:hd], (turn[0], turn[1]), root)
    values = (kv_rows[:, hd:2 * hd] * root).astype(BF16)
    scores = lax.dot_general(queries, keys, (((1,), (1,)), ((), ())), preferred_element_type=F32)
    scores = scores * ((d / n_dp) ** (-0.5) / 50.0)
    expd = jnp.exp(50.0 * jnp.tanh(scores)) * seen[...]
    denominator = jnp.sum(expd, axis=-1, keepdims=True)
    numer = jnp.dot(expd.astype(BF16), values, preferred_element_type=F32)
    attended = (numer / denominator).astype(BF16)
    wo_copy.wait_recv()
    both = jnp.concatenate([attended[0:mine], attended[mine:2 * mine]], axis=1)

    def ring_copy(way, step, k):
        goal = device(pos + step_of[way])
        if hops(way, k) - step + 1 > cross:
            goal = {"dp": jnp.where(from_middle[1 - way], mate["dp"], goal["dp"])}
        return remote(ring_out.at[k, way * far + step - 1], ring_in.at[k, way * far + step - 1],
                      ring_done.at[0], ring_sem.at[place_of(way, step, k)], goal)

    def launch(way, step, k, total):
        ring_out[k, way * far + step - 1] = total.astype(BF16)
        ring_copy(way, step, k).start()

    for k in MIXED:
        terms = jnp.dot(both, wo[:, k * kd:(k + 1) * kd], preferred_element_type=F32)
        part[k] = terms.reshape(chips, toks, kd)
        way = 0 if hops(0, k) == far else 1
        launch(way, 1, k, part[k, chips - 1])
    for j in range(half):
        for way in range(2):
            k = SORTED[way][half + j]
            launch(way, 1, k, part[k, slot(1 - way, hops(way, k))])
    for j in range(mb):
        owner, number = origin(secs, sec, mb, act_pp, j)
        for k in range(CHUNKS):
            moved[j, :, k * kd:(k + 1) * kd] = actrecv[k][owner, number]

    waited, early = set(), set()

    def take(way, step, k):
        copy = ring_copy(way, step, k)
        if (way, step, k) in early:
            pl.when(jnp.logical_not(from_middle[way]))(copy.wait_recv)
        else:
            copy.wait_recv()
        waited.add((way, step, k))
        return ring_in[k, way * far + step - 1].astype(F32)

    def relay(way, step, k):
        left = hops(way, k) - step
        came = take(way, step, k)
        if left + 1 > cross:
            came = jnp.where(from_middle[way], 0.0, came)
        target = slot(1 - way, left)
        there = far + 1 - left
        if cross < there <= hops(1 - way, k):
            other_step = hops(1 - way, k) - there + 1
            late = (1 - way, other_step, k) not in waited
            if late:
                early.add((1 - way, other_step, k))

            @pl.when(from_middle[1 - way])
            def _():
                if late:
                    ring_copy(1 - way, other_step, k).wait_recv()
                part[k, target] = part[k, target] + ring_in[k, (1 - way) * far + other_step - 1].astype(F32)

        launch(way, step + 1, k, part[k, target] + came)

    for step in range(1, far):
        for group in range(2):
            for j in range(half):
                for way in range(2):
                    k = SORTED[way][group * half + j]
                    if step < hops(way, k):
                        relay(way, step, k)

    others = pl.ds(0, n_dp - 1)
    all_blocks = remote(sacc.at[others], racc.at[others], blk_sem.at[0], blk_sem.at[1], partner)
    all_blocks.wait_recv()
    scale_sum = jnp.sum(racc[:, 0, :, pl.ds(d, LANES)].astype(F32), axis=0)
    factor = n_dp / jnp.sum(jnp.sum(scale_sum, axis=0, keepdims=True), axis=1, keepdims=True)

    def unpack(b, carry):
        owner, number = origin(blks, me, blk, blk_pp, b)
        accout[b] = racc[owner, number, :, pl.ds(0, d)].astype(F32) * factor
        return carry

    lax.fori_loop(0, blk, unpack, 0)

    pieces = []
    for k in range(CHUNKS):
        total = part[k, 0]
        for way in range(2):
            total = total + take(way, hops(way, k), k)
        pieces.append(total)
    loads["post"].wait()
    square = sum(jnp.sum(t * t, axis=-1, keepdims=True) for t in pieces)
    scale = lax.rsqrt(square / d + 1e-06)
    for k in range(CHUNKS):
        cols = slice(k * kd, (k + 1) * kd)
        outbuf[0, :, cols] = (
            moved[0, :, cols].astype(F32) + pieces[k] * scale * post[:, cols]
        ).astype(BF16)
    for copy in (weights, wo_copy, all_blocks):
        copy.wait_send()
    for o in range(1, n_sec):
        q = (sec + o) % n_sec
        remote(stage.at[q], stage.at[q], act_out.at[o - 1], act_sem.at[o - 1, 0], {"section": q}).wait_send()
    for i, span in enumerate((pl.ds(0, CHUNKS - 1), pl.ds(CHUNKS - 1, 1))):
        for slots, sem in ((chips, fwd_out.at[i]), (chips - 1, ag_out.at[i])):
            block = gath.at[span, core, pl.ds(0, slots), :, pl.ds(0, width(i * (CHUNKS - 1)))]
            remote(block, block, sem, fwd_sem.at[0, 0], partner).wait_send()
    block = ring_out.at[:, pl.ds(0, chips - 1)]
    remote(block, block, ring_done.at[0], fwd_sem.at[0, 0], partner).wait_send()


def write_out(moved, accout, outbuf, moved_hbm, newacc_hbm, check_hbm, sems):
    copies = [
        pltpu.make_async_copy(src, dst, sems.at[i])
        for i, (src, dst) in enumerate([(accout, newacc_hbm), (moved, moved_hbm), (outbuf, check_hbm)])
    ]
    for copy in copies:
        copy.start()
    for copy in copies:
        copy.wait()


def make_on_device(n_sec, n_dp):
    def on_device(activations, section_sources, accumulators, block_sources, loss_terms,
                  pre_gain, query_weight, keyval_weight, output_weight, post_gain):
        mb, toks, d = activations.shape
        blk, brows, _ = accumulators.shape
        hd = query_weight.shape[2]
        chips, far, kd, length = n_dp // 2, n_dp // 4, d // CHUNKS, n_dp * toks
        rot = jnp.asarray(rotary_tables(length, hd).reshape(2, chips, 2, toks, hd))
        smem = pltpu.SMEM
        in_hbm = pl.BlockSpec(memory_space=pltpu.HBM)
        vmem = pl.BlockSpec(memory_space=pltpu.VMEM)
        dma = pltpu.SemaphoreType.DMA
        act_pp, blk_pp = mb // n_sec, blk // n_dp
        out_bytes = activations.size * 2 + accumulators.size * 4 + toks * d * 2
        held = pl.pallas_call(
            functools.partial(kernel, (n_sec, n_dp)),
            out_shape=(
                pltpu.VMEM(activations.shape, BF16),
                pltpu.VMEM(accumulators.shape, F32),
                pltpu.VMEM((1, toks, d), BF16),
            ),
            in_specs=[in_hbm] * 11,
            out_specs=(vmem,) * 3,
            scratch_shapes=[
                smem(section_sources.shape, jnp.int32),
                smem(block_sources.shape, jnp.int32),
                smem((1, 1), F32),
                pltpu.VMEM(activations.shape, BF16),
                pltpu.VMEM(accumulators.shape, F32),
                pltpu.VMEM((1, d), F32),
                pltpu.VMEM((1, d), F32),
                pltpu.VMEM(rot.shape, F32),
                pltpu.VMEM((2, 2, chips, toks, hd), F32),
                pltpu.VMEM((length, length), F32),
                pltpu.VMEM((d, 4 * hd), BF16),
                pltpu.VMEM((2 * hd, d), BF16),
                pltpu.VMEM((n_sec, CHUNKS, act_pp, toks, kd), BF16),
                (pltpu.VMEM((n_sec, act_pp, toks, kd), BF16),) * CHUNKS,
                pltpu.VMEM((n_dp, blk_pp, brows, d + LANES), BF16),
                pltpu.VMEM((n_dp, blk_pp, brows, d + LANES), BF16),
                pltpu.VMEM((CHUNKS, 2, chips, toks, kd + LANES), BF16),
                pltpu.VMEM((chips, toks, 2 * hd), F32),
                pltpu.VMEM((2, chips, toks, 2 * hd), F32),
                pltpu.VMEM((CHUNKS, chips, toks, kd), F32),
                pltpu.VMEM((CHUNKS, 2 * far, toks, kd), BF16),
                pltpu.VMEM((CHUNKS, 2 * far, toks, kd), BF16),
                pltpu.SemaphoreType.REGULAR,
                dma((9,)),
                dma((n_sec - 1,)),
                dma((n_sec - 1, CHUNKS)),
                dma((4,)),
                dma((2,)),
                dma((2,)),
                dma(((2 * far - 1) * CHUNKS,)),
                dma((2,)),
                dma((2, CHUNKS)),
                dma((1,)),
                dma(((2 * far - 1) * CHUNKS,)),
            ],
            compiler_params=pltpu.CompilerParams(
                collective_id=0, has_side_effects=True, vmem_limit_bytes=VMEM_BYTES - 2**16 - out_bytes
            ),
        )(section_sources, block_sources, loss_terms, activations, accumulators,
          pre_gain, query_weight, keyval_weight, output_weight, post_gain, rot)
        return pl.pallas_call(
            write_out,
            out_shape=(
                jax.ShapeDtypeStruct(activations.shape, BF16),
                jax.ShapeDtypeStruct(accumulators.shape, F32),
                jax.ShapeDtypeStruct((1, toks, d), BF16),
            ),
            in_specs=[vmem] * 3,
            out_specs=(in_hbm,) * 3,
            scratch_shapes=[dma((3,))],
            compiler_params=pltpu.CompilerParams(vmem_limit_bytes=4 * 2**20),
        )(*held)

    return on_device


def solution(mesh):
    placed = (
        P("section", "dp", None),
        P(),
        P("dp", "section", None),
        P(),
        P("section", "dp"),
        P("section", None),
        P("section", None, "dp"),
        P("section", None, "dp"),
        P("section", "dp", None),
        P("section", None),
    )
    return jax.shard_map(
        make_on_device(mesh.shape["section"], mesh.shape["dp"]),
        mesh=mesh,
        in_specs=placed,
        out_specs=(P("section", "dp", None), P("dp", "section", None), P("section", "dp", None)),
        check_vma=False,
    )
```

```python
import functools

import jax
import jax.numpy as jnp
import numpy as np
from jax import lax
from jax.experimental import pallas as pl
from jax.experimental.pallas import tpu as pltpu
from jax.sharding import PartitionSpec as P

LANES = 128
VMEM_BYTES = 67043328
CHUNKS = 6
MIXED = (0, 3, 1, 4, 2, 5)
AHEAD = ((0, 1, 3, 2, 4, 5), (3, 0, 4, 1, 5, 2))
SORTED = ((0, 1, 2, 3, 4, 5), (3, 4, 5, 0, 1, 2))
F32 = jnp.float32
BF16 = jnp.bfloat16


def pick(table, own, groups, per_group, peer, rank):
    first, start = peer * per_group, own * per_group
    seen = found = jnp.int32(0)
    for j in range(per_group):
        offset = table[first + j] - start
        hit = (offset >= 0) & (offset < per_group)
        if per_group == groups:
            found = jnp.where(hit, offset, found)
        else:
            found = jnp.where(hit & (seen == rank), offset, found)
            seen = seen + hit.astype(jnp.int32)
    return found


def origin(table, own, per_group, per_peer, entry):
    owner = table[own * per_group + entry] // per_group
    if per_peer == 1:
        return owner, 0

    def visit(j, seen):
        same = table[own * per_group + j] // per_group == owner
        return seen + same.astype(jnp.int32) * (j < entry).astype(jnp.int32)

    return owner, lax.fori_loop(0, per_group, visit, jnp.int32(0))


def rotary_tables(length, width):
    half = width // 2
    freqs = np.float32(10000.0) ** (np.float32(-2.0) * np.arange(half, dtype=np.float32) / np.float32(width))
    angles = np.arange(length, dtype=np.float32)[:, None] * freqs.astype(np.float32)[None, :]
    cosine, sine = np.cos(angles.astype(np.float64)), np.sin(angles.astype(np.float64))
    return np.stack(
        [np.concatenate([cosine, cosine], 1), np.concatenate([-sine, sine], 1)]
    ).astype(np.float32)


def kernel(
    dims,
    secs_hbm, blks_hbm, loss_hbm, act_hbm, acc_hbm, pre_hbm, wq_hbm, wkv_hbm, wo_hbm, post_hbm, rot_hbm,
    moved, accout, outbuf,
    secs, blks, loss, act, acc, pre, post, rot, turn, seen, w, wo,
    stage, actrecv, sacc, racc,
    gath, qs, kvs, part, ring_in, ring_out,
    ready, load_sem, act_out, act_sem, w_sem, blk_sem, ag_out, ag_sem, fwd_out, fwd_sem, ring_done, ring_sem,
):
    n_sec, n_dp = dims
    mb, toks, d = act.shape
    blk, brows, _ = acc.shape
    act_pp, blk_pp = mb // n_sec, blk // n_dp
    chips = n_dp // 2
    far = chips // 2
    kd = d // CHUNKS
    length = n_dp * toks
    hd = wq_hbm.shape[2]
    sec, me = lax.axis_index("section"), lax.axis_index("dp")
    core, chip = me % 2, me // 2
    side, rung = chip % 2, chip // 2
    pos = rung * (1 - side) + (chips - 1 - rung) * side

    def chip_at(p):
        q = (p + 2 * chips) % chips
        s = q // (chips // 2)
        return 2 * (q * (1 - s) + (chips - 1 - q) * s) + s

    def device(p):
        return {"dp": 2 * chip_at(p) + 1 - core}

    partner = {"dp": me + 1 - 2 * core}
    mate = {"dp": 2 * (2 * rung + 1 - side) + 1 - core}
    cross = far // 2
    from_middle = ((pos == cross) | (pos == chips - cross), (pos == cross - 1) | (pos == chips - cross - 1))

    def remote(src, dst, send_sem, recv_sem, dev):
        return pltpu.make_async_remote_copy(
            src_ref=src, dst_ref=dst, send_sem=send_sem, recv_sem=recv_sem,
            device_id=dev, device_id_type=pl.DeviceIdType.MESH,
        )

    barrier = pltpu.get_barrier_semaphore()
    for o in range(1, n_sec):
        pl.semaphore_signal(barrier, inc=1, device_id={"section": (sec + o) % n_sec},
                            device_id_type=pl.DeviceIdType.MESH)
    def same(dev):
        return {"dp": dev["dp"] + 2 * core - 1}

    for near in (same(device(pos + 1)), same(device(pos - 1)), partner, same(mate)):
        pl.semaphore_signal(barrier, inc=1, device_id=near, device_id_type=pl.DeviceIdType.MESH)

    kv_cols = pl.ds(pl.multiple_of(2 * hd + core * hd, LANES), hd)
    q_cols = pl.ds(pl.multiple_of(core * hd, LANES), hd)
    wo_rows = pl.ds(pl.multiple_of(core * hd, LANES), hd)
    names = ("secs", "act", "pre", "wkv", "blks", "loss", "acc", "rot", "post", "wo", "wq")
    pairs = [
        (secs_hbm, secs), (act_hbm, act), (pre_hbm, pre), (wkv_hbm.at[0], w.at[:, kv_cols]),
        (blks_hbm, blks), (loss_hbm, loss), (acc_hbm, acc), (rot_hbm, rot), (post_hbm, post),
        (wo_hbm.at[0], wo.at[wo_rows]), (wq_hbm.at[0], w.at[:, q_cols]),
    ]
    loads = {
        name: pltpu.make_async_copy(src, dst, load_sem.at[names.index("wkv") if name in ("wq", "wo") else i])
        for i, (name, (src, dst)) in enumerate(zip(names, pairs))
    }
    for name in ("secs", "act", "blks", "loss", "acc", "pre", "wkv", "wq", "wo", "rot", "post"):
        loads[name].start()

    loads["secs"].wait()
    loads["act"].wait()
    for q in range(n_sec):
        for r in range(act_pp):
            block = act[pick(secs, sec, n_sec, mb, q, r)]
            for k in range(CHUNKS):
                stage[q, k, r] = block[:, k * kd:(k + 1) * kd]
    pl.semaphore_wait(barrier, n_sec - 1 + 4)
    pl.semaphore_signal(ready, inc=1, device_id=partner, device_id_type=pl.DeviceIdType.MESH)
    act_copies = [[] for _ in range(CHUNKS)]
    for k in MIXED:
        for o in range(1, n_sec):
            q = (sec + o) % n_sec
            copy = remote(stage.at[q, k], actrecv[k].at[sec], act_out.at[o - 1], act_sem.at[o - 1, k], {"section": q})
            copy.start()
            act_copies[k].append(copy)
    for k in range(CHUNKS):
        actrecv[k][sec] = stage[sec, k]

    for name in ("acc", "blks", "loss"):
        loads[name].wait()
    term = jnp.full((brows, LANES), loss[0, 0], F32)
    high = term.astype(BF16).astype(F32)
    lane = lax.broadcasted_iota(jnp.int32, (brows, LANES), 1)
    row = lax.broadcasted_iota(jnp.int32, (brows, LANES), 0)
    tail = jnp.where(row > 0, 0.0, jnp.where(lane == 0, high, jnp.where(lane == 1, term - high, 0.0)))

    def pack(p, carry):
        for r in range(blk_pp):
            sacc[p, r, :, pl.ds(0, d)] = acc[pick(blks, me, n_dp, blk, p, r)].astype(BF16)
            sacc[p, r, :, pl.ds(d, LANES)] = tail.astype(BF16)
        return carry

    def pack_near(i, carry):
        j = (i // 2 + 1) % chips
        return pack(2 * chip_at(pos + (j + 1) // 2 * (1 - 2 * (j % 2))) + i % 2, carry)

    other = me + 1 - 2 * core
    step_of = (1, -1)

    def send_block(peer):
        remote(sacc.at[peer], racc.at[me], blk_sem.at[0], blk_sem.at[1], {"dp": peer}).start()

    def send_blocks(places):
        for way, hop in places:
            for c in range(2):
                send_block(2 * chip_at(pos + step_of[way] * hop) + (core + c) % 2)

    lax.fori_loop(0, 4, pack_near, 0)
    pl.semaphore_wait(ready, 1)
    send_blocks([(0, 1), (1, 1)])
    some = n_dp // 16
    lax.fori_loop(4, n_dp - 4 * some, pack_near, 0)
    mine = chips * toks

    def token_at(row, first_core):
        block = row // toks
        j = block % chips
        p = (pos + (j + 1) // 2 * (1 - 2 * (j % 2)) + 2 * chips) % chips
        s = p // (chips // 2)
        return (2 * (2 * (p * (1 - s) + (chips - 1 - p) * s) + s) + (first_core + block // chips + (j + 1) // 2) % 2) * toks + row % toks

    query_token = token_at(lax.broadcasted_iota(jnp.int32, (2 * mine, 1), 0) % mine, core)
    key_token = token_at(lax.broadcasted_iota(jnp.int32, (1, length), 1), 0)
    seen[...] = (key_token <= query_token).astype(F32)

    loads["pre"].wait()

    def hops(way, k):
        return far if (k < CHUNKS // 2) == (way == 0) else far - 1


    def width(k):
        return kd + LANES if k == MIXED[-1] else kd

    def place_of(way, hop, k):
        return (hop - 1) * 2 * CHUNKS + (way * CHUNKS if hop < far else 0) + k

    def last(k):
        return 1 if k == MIXED[-1] else 0

    def slot(way, hop):
        return 0 if hop == 0 else min(2 * hop - 1 + way, chips - 1)

    def blocks_of(k, c, slots):
        return gath.at[k, c, slots, :, pl.ds(0, width(k))]

    def gather_copy(way, hop, k):
        return remote(blocks_of(k, core, slot(way, hop - 1)), blocks_of(k, 1 - core, slot(way, hop)),
                      ag_out.at[last(k)], ag_sem.at[place_of(way, hop, k)], device(pos + step_of[way]))

    def forward(way, hop, k):
        if hop < hops(way, k):
            if hop < cross:
                gather_copy(way, hop + 1, k).start()
            else:
                pl.when(jnp.logical_not(from_middle[1 - way]))(gather_copy(way, hop + 1, k).start)
        there = far + 1 - hop
        if cross < there <= hops(1 - way, k):
            across = remote(blocks_of(k, core, slot(way, hop)), blocks_of(k, 1 - core, slot(1 - way, there)),
                            ag_out.at[last(k)], ag_sem.at[place_of(1 - way, there, k)], mate)
            pl.when(from_middle[way])(across.start)

    near = 2 * (far - 2) + 1
    spans = (slice(0, near), slice(near, chips))

    def pass_on(j, k):
        block = blocks_of(k, core, j)
        remote(block, block, fwd_out.at[last(k)], fwd_sem.at[0 if j < near else 1, k], partner).start()

    square = jnp.zeros((toks, 1), F32)
    for k in MIXED:
        for copy in act_copies[k]:
            copy.wait_recv()
        owner, number = origin(secs, sec, mb, act_pp, 0)
        piece = actrecv[k][owner, number].astype(F32)
        square = square + jnp.sum(piece * piece, axis=-1, keepdims=True)
        gath[k, core, 0, :, pl.ds(0, kd)] = (piece * pre[:, k * kd:(k + 1) * kd]).astype(BF16)
        if k == MIXED[-1]:
            root = jnp.broadcast_to(lax.rsqrt(square / d + 1e-06), (toks, LANES))
            high = root.astype(BF16).astype(F32)
            lane = lax.broadcasted_iota(jnp.int32, (toks, LANES), 1)
            gath[k, core, 0, :, pl.ds(kd, LANES)] = jnp.where(
                lane == 0, high, jnp.where(lane == 1, root - high, 0.0)).astype(BF16)
        for way in range(2):
            gather_copy(way, 1, k).start()
        pass_on(0, k)


    def project(ks, part_of, fresh):
        span = spans[part_of]
        count = span.stop - span.start

        def add(ref, index, cores, cols):
            terms = sum(
                jnp.dot(gath[k, cores, span, :, pl.ds(0, kd)].reshape(-1, kd), w[k * kd:(k + 1) * kd, cols],
                        preferred_element_type=F32)
                for k in ks
            ).reshape(ref[index].shape)
            ref[index] = terms if fresh else ref[index] + terms

        add(qs, span, core, slice(0, 2 * hd))
        for k in ks:
            block = blocks_of(k, 1 - core, pl.ds(span.start, count))
            remote(block, block, fwd_out.at[0], fwd_sem.at[part_of, k], partner).wait_recv()
        add(kvs, (slice(None), span), slice(None), slice(2 * hd, 4 * hd))

    three = w.at[:, pl.ds(0, 3 * hd)]
    weights_loaded = load_sem.at[names.index("wkv")]
    remote(three, three, weights_loaded, weights_loaded, partner).wait_recv()
    two = w.at[:, pl.ds(0, 2 * hd)]
    weights = remote(two, two, w_sem.at[0], w_sem.at[1], partner)
    wo_copy = remote(wo.at[wo_rows], wo.at[wo_rows], w_sem.at[2], w_sem.at[3], partner)

    def share(ref, i):
        remote(ref, ref, w_sem.at[i], w_sem.at[i + 1], partner).start()

    loads["rot"].wait()
    for j in range(chips):
        place = chip_at(pos + (j + 1) // 2 * (1 - 2 * (j % 2)))
        for c in range(2):
            for t in range(2):
                turn[t, c, j] = rot[t, place, (c + (j + 1) // 2) % 2]

    half = CHUNKS // 2
    for hop in range(1, far + 1):
        order = (MIXED, MIXED) if hop == 1 else AHEAD if hop < far else SORTED
        for i in range(CHUNKS if hop < far else half):
            for way in range(2):
                k = order[way][i]
                gather_copy(way, hop, k).wait_recv()
                forward(way, hop, k)
                pass_on(slot(way, hop), k)
            if hop == 1:
                rows = pl.ds(i * kd, kd)
                share(w.at[rows, kv_cols], 0)
                share(w.at[rows, q_cols], 0)
                if i < 4:
                    lax.fori_loop(n_dp - (4 - i) * some, n_dp - (3 - i) * some, pack_near, 0)
                elif i == 4:
                    racc[me] = sacc[me]
                    send_block(other)
            if hop == 2:
                share(wo.at[wo_rows, pl.ds(i * kd, kd)], 2)
            if hop == far - 1 and i == CHUNKS - 1:
                send_blocks([(way, far - h) for h in range(1, far - 1) for way in range(2)])
            if hop == far - 1 and i == 1:
                weights.wait_recv()
            if hop == far - 1 and i % 2 == 1:
                project(MIXED[i - 1:i + 1], 0, i == 1)
            if hop == far and i > 0:
                project((i - 1, half + i - 1), 1, i == 1)
            if hop == far and i == 0:
                send_blocks([(0, far)])
    project((half - 1, CHUNKS - 1), 1, False)

    def root_of(parts):
        return jnp.sum(parts.reshape(-1, LANES).astype(F32), axis=-1, keepdims=True)

    def turned(v, tables, root):
        return (v * (tables[0].reshape(-1, hd) * root) + pltpu.roll(v, hd // 2, 1) * (tables[1].reshape(-1, hd) * root)).astype(BF16)

    root = root_of(gath[CHUNKS - 1, :, :, :, pl.ds(kd, LANES)])
    own_root = root_of(gath[CHUNKS - 1, core, :, :, pl.ds(kd, LANES)])
    own_turn = turn[0, core], turn[1, core]

    q_rows = qs[...].reshape(mine, 2 * hd)
    kv_rows = kvs[...].reshape(length, 2 * hd)
    queries = jnp.concatenate([turned(q_rows[:, 0:hd], own_turn, own_root), turned(q_rows[:, hd:2 * hd], own_turn, own_root)], axis=0)
    keys = turned(kv_rows[:, 0:hd], (turn[0], turn[1]), root)
    values = (kv_rows[:, hd:2 * hd] * root).astype(BF16)
    scores = lax.dot_general(queries, keys, (((1,), (1,)), ((), ())), preferred_element_type=F32)
    scores = scores * ((d / n_dp) ** (-0.5) / 50.0)
    expd = jnp.exp(50.0 * jnp.tanh(scores)) * seen[...]
    denominator = jnp.sum(expd, axis=-1, keepdims=True)
    numer = jnp.dot(expd.astype(BF16), values, preferred_element_type=F32)
    attended = (numer / denominator).astype(BF16)
    wo_copy.wait_recv()
    both = jnp.concatenate([attended[0:mine], attended[mine:2 * mine]], axis=1)

    def ring_copy(way, step, k):
        goal = device(pos + step_of[way])
        if hops(way, k) - step + 1 > cross:
            goal = {"dp": jnp.where(from_middle[1 - way], mate["dp"], goal["dp"])}
        return remote(ring_out.at[k, way * far + step - 1], ring_in.at[k, way * far + step - 1],
                      ring_done.at[0], ring_sem.at[place_of(way, step, k)], goal)

    def crossing(way, step, k):
        return hops(way, k) - step + 1 > cross

    def launch(way, step, k, total):
        ring_out[k, way * far + step - 1] = total.astype(BF16)
        start = ring_copy(way, step, k).start
        if step == 1 and crossing(way, 1, k):
            pl.when(jnp.logical_not(from_middle[1 - way]))(start)
        else:
            start()

    for k in MIXED:
        terms = jnp.dot(both, wo[:, k * kd:(k + 1) * kd], preferred_element_type=F32)
        part[k] = terms.reshape(chips, toks, kd)
        way = 0 if hops(0, k) == far else 1
        launch(way, 1, k, part[k, chips - 1])
    for j in range(half):
        for way in range(2):
            k = SORTED[way][half + j]
            launch(way, 1, k, part[k, slot(1 - way, hops(way, k))])
    for j in range(mb):
        owner, number = origin(secs, sec, mb, act_pp, j)
        for k in range(CHUNKS):
            moved[j, :, k * kd:(k + 1) * kd] = actrecv[k][owner, number]

    def take(way, step, k):
        ring_copy(way, step, k).wait_recv()
        return ring_in[k, way * far + step - 1].astype(F32)

    def relay(way, step, k):
        left = hops(way, k) - step
        target = slot(1 - way, left)
        there = far + 1 - left
        if crossing(way, step, k):
            @pl.when(jnp.logical_not(from_middle[way]))
            def _():
                part[k, target] = part[k, target] + take(way, step, k)
        if cross < there <= hops(1 - way, k):
            @pl.when(from_middle[1 - way])
            def _():
                part[k, target] = part[k, target] + take(1 - way, hops(1 - way, k) - there + 1, k)
        total = part[k, target]
        launch(way, step + 1, k, total if crossing(way, step, k) else total + take(way, step, k))

    for step in range(1, far):
        for group in range(2):
            for j in range(half):
                for way in range(2):
                    k = SORTED[way][group * half + j]
                    if step < hops(way, k):
                        relay(way, step, k)
            if step == 1 and group == 0:
                for way in range(2):
                    for k in SORTED[way][half:] + SORTED[way][:half]:
                        pl.when(from_middle[1 - way])(ring_copy(way, 1, k).start)

    others = pl.ds(0, n_dp - 1)
    all_blocks = remote(sacc.at[others], racc.at[others], blk_sem.at[0], blk_sem.at[1], partner)
    all_blocks.wait_recv()
    scale_sum = jnp.sum(racc[:, 0, :, pl.ds(d, LANES)].astype(F32), axis=0)
    factor = n_dp / jnp.sum(jnp.sum(scale_sum, axis=0, keepdims=True), axis=1, keepdims=True)

    def unpack(b, carry):
        owner, number = origin(blks, me, blk, blk_pp, b)
        accout[b] = racc[owner, number, :, pl.ds(0, d)].astype(F32) * factor
        return carry

    lax.fori_loop(0, blk, unpack, 0)

    pieces = []
    for k in range(CHUNKS):
        total = part[k, 0]
        for way in range(2):
            total = total + take(way, hops(way, k), k)
        pieces.append(total)
    loads["post"].wait()
    square = sum(jnp.sum(t * t, axis=-1, keepdims=True) for t in pieces)
    scale = lax.rsqrt(square / d + 1e-06)
    for k in range(CHUNKS):
        cols = slice(k * kd, (k + 1) * kd)
        outbuf[0, :, cols] = (
            moved[0, :, cols].astype(F32) + pieces[k] * scale * post[:, cols]
        ).astype(BF16)
    for copy in (weights, wo_copy, all_blocks):
        copy.wait_send()
    for o in range(1, n_sec):
        q = (sec + o) % n_sec
        remote(stage.at[q], stage.at[q], act_out.at[o - 1], act_sem.at[o - 1, 0], {"section": q}).wait_send()
    for i, span in enumerate((pl.ds(0, CHUNKS - 1), pl.ds(CHUNKS - 1, 1))):
        for slots, sem in ((chips, fwd_out.at[i]), (chips - 1, ag_out.at[i])):
            block = gath.at[span, core, pl.ds(0, slots), :, pl.ds(0, width(i * (CHUNKS - 1)))]
            remote(block, block, sem, fwd_sem.at[0, 0], partner).wait_send()
    block = ring_out.at[:, pl.ds(0, chips - 1)]
    remote(block, block, ring_done.at[0], fwd_sem.at[0, 0], partner).wait_send()


def write_out(moved, accout, outbuf, moved_hbm, newacc_hbm, check_hbm, sems):
    copies = [
        pltpu.make_async_copy(src, dst, sems.at[i])
        for i, (src, dst) in enumerate([(accout, newacc_hbm), (moved, moved_hbm), (outbuf, check_hbm)])
    ]
    for copy in copies:
        copy.start()
    for copy in copies:
        copy.wait()


def make_on_device(n_sec, n_dp):
    def on_device(activations, section_sources, accumulators, block_sources, loss_terms,
                  pre_gain, query_weight, keyval_weight, output_weight, post_gain):
        mb, toks, d = activations.shape
        blk, brows, _ = accumulators.shape
        hd = query_weight.shape[2]
        chips, far, kd, length = n_dp // 2, n_dp // 4, d // CHUNKS, n_dp * toks
        rot = jnp.asarray(rotary_tables(length, hd).reshape(2, chips, 2, toks, hd))
        smem = pltpu.SMEM
        in_hbm = pl.BlockSpec(memory_space=pltpu.HBM)
        vmem = pl.BlockSpec(memory_space=pltpu.VMEM)
        dma = pltpu.SemaphoreType.DMA
        act_pp, blk_pp = mb // n_sec, blk // n_dp
        out_bytes = activations.size * 2 + accumulators.size * 4 + toks * d * 2
        held = pl.pallas_call(
            functools.partial(kernel, (n_sec, n_dp)),
            out_shape=(
                pltpu.VMEM(activations.shape, BF16),
                pltpu.VMEM(accumulators.shape, F32),
                pltpu.VMEM((1, toks, d), BF16),
            ),
            in_specs=[in_hbm] * 11,
            out_specs=(vmem,) * 3,
            scratch_shapes=[
                smem(section_sources.shape, jnp.int32),
                smem(block_sources.shape, jnp.int32),
                smem((1, 1), F32),
                pltpu.VMEM(activations.shape, BF16),
                pltpu.VMEM(accumulators.shape, F32),
                pltpu.VMEM((1, d), F32),
                pltpu.VMEM((1, d), F32),
                pltpu.VMEM(rot.shape, F32),
                pltpu.VMEM((2, 2, chips, toks, hd), F32),
                pltpu.VMEM((length, length), F32),
                pltpu.VMEM((d, 4 * hd), BF16),
                pltpu.VMEM((2 * hd, d), BF16),
                pltpu.VMEM((n_sec, CHUNKS, act_pp, toks, kd), BF16),
                (pltpu.VMEM((n_sec, act_pp, toks, kd), BF16),) * CHUNKS,
                pltpu.VMEM((n_dp, blk_pp, brows, d + LANES), BF16),
                pltpu.VMEM((n_dp, blk_pp, brows, d + LANES), BF16),
                pltpu.VMEM((CHUNKS, 2, chips, toks, kd + LANES), BF16),
                pltpu.VMEM((chips, toks, 2 * hd), F32),
                pltpu.VMEM((2, chips, toks, 2 * hd), F32),
                pltpu.VMEM((CHUNKS, chips, toks, kd), F32),
                pltpu.VMEM((CHUNKS, 2 * far, toks, kd), BF16),
                pltpu.VMEM((CHUNKS, 2 * far, toks, kd), BF16),
                pltpu.SemaphoreType.REGULAR,
                dma((9,)),
                dma((n_sec - 1,)),
                dma((n_sec - 1, CHUNKS)),
                dma((4,)),
                dma((2,)),
                dma((2,)),
                dma(((2 * far - 1) * CHUNKS,)),
                dma((2,)),
                dma((2, CHUNKS)),
                dma((1,)),
                dma(((2 * far - 1) * CHUNKS,)),
            ],
            compiler_params=pltpu.CompilerParams(
                collective_id=0, has_side_effects=True, vmem_limit_bytes=VMEM_BYTES - 2**16 - out_bytes
            ),
        )(section_sources, block_sources, loss_terms, activations, accumulators,
          pre_gain, query_weight, keyval_weight, output_weight, post_gain, rot)
        return pl.pallas_call(
            write_out,
            out_shape=(
                jax.ShapeDtypeStruct(activations.shape, BF16),
                jax.ShapeDtypeStruct(accumulators.shape, F32),
                jax.ShapeDtypeStruct((1, toks, d), BF16),
            ),
            in_specs=[vmem] * 3,
            out_specs=(in_hbm,) * 3,
            scratch_shapes=[dma((3,))],
            compiler_params=pltpu.CompilerParams(vmem_limit_bytes=4 * 2**20),
        )(*held)

    return on_device


def solution(mesh):
    placed = (
        P("section", "dp", None),
        P(),
        P("dp", "section", None),
        P(),
        P("section", "dp"),
        P("section", None),
        P("section", None, "dp"),
        P("section", None, "dp"),
        P("section", "dp", None),
        P("section", None),
    )
    return jax.shard_map(
        make_on_device(mesh.shape["section"], mesh.shape["dp"]),
        mesh=mesh,
        in_specs=placed,
        out_specs=(P("section", "dp", None), P("dp", "section", None), P("section", "dp", None)),
        check_vma=False,
    )
```

```python
import functools

import jax
import jax.numpy as jnp
import numpy as np
from jax import lax
from jax.experimental import pallas as pl
from jax.experimental.pallas import tpu as pltpu
from jax.sharding import PartitionSpec as P

LANES = 128
VMEM_BYTES = 67043328
CHUNKS = 6
MIXED = (0, 3, 1, 4, 2, 5)
AHEAD = ((0, 1, 3, 2, 4, 5), (3, 0, 4, 1, 5, 2))
SORTED = ((0, 1, 2, 3, 4, 5), (3, 4, 5, 0, 1, 2))
F32 = jnp.float32
BF16 = jnp.bfloat16


def pick(table, own, groups, per_group, peer, rank):
    first, start = peer * per_group, own * per_group
    seen = found = jnp.int32(0)
    for j in range(per_group):
        offset = table[first + j] - start
        hit = (offset >= 0) & (offset < per_group)
        if per_group == groups:
            found = jnp.where(hit, offset, found)
        else:
            found = jnp.where(hit & (seen == rank), offset, found)
            seen = seen + hit.astype(jnp.int32)
    return found


def origin(table, own, per_group, per_peer, entry):
    owner = table[own * per_group + entry] // per_group
    if per_peer == 1:
        return owner, 0

    def visit(j, seen):
        same = table[own * per_group + j] // per_group == owner
        return seen + same.astype(jnp.int32) * (j < entry).astype(jnp.int32)

    return owner, lax.fori_loop(0, per_group, visit, jnp.int32(0))


def rotary_tables(length, width):
    half = width // 2
    freqs = np.float32(10000.0) ** (np.float32(-2.0) * np.arange(half, dtype=np.float32) / np.float32(width))
    angles = np.arange(length, dtype=np.float32)[:, None] * freqs.astype(np.float32)[None, :]
    cosine, sine = np.cos(angles.astype(np.float64)), np.sin(angles.astype(np.float64))
    return np.stack(
        [np.concatenate([cosine, cosine], 1), np.concatenate([-sine, sine], 1)]
    ).astype(np.float32)


def kernel(
    dims,
    secs_hbm, blks_hbm, loss_hbm, act_hbm, acc_hbm, pre_hbm, wq_hbm, wkv_hbm, wo_hbm, post_hbm, rot_hbm,
    moved, accout, outbuf,
    secs, blks, loss, act, acc, pre, post, rot, turn, seen, w, wo,
    stage, actrecv, sacc, racc,
    gath, qs, kvs, part, ring_in, ring_out,
    ready, load_sem, act_out, act_sem, w_sem, blk_sem, ag_out, ag_sem, fwd_out, fwd_sem, ring_done, ring_sem,
):
    n_sec, n_dp = dims
    mb, toks, d = act.shape
    blk, brows, _ = acc.shape
    act_pp, blk_pp = mb // n_sec, blk // n_dp
    chips = n_dp // 2
    far = chips // 2
    kd = d // CHUNKS
    half = CHUNKS // 2
    length = n_dp * toks
    hd = wq_hbm.shape[2]
    sec, me = lax.axis_index("section"), lax.axis_index("dp")
    core, chip = me % 2, me // 2
    side, rung = chip % 2, chip // 2
    pos = rung * (1 - side) + (chips - 1 - rung) * side

    def chip_at(p):
        q = (p + 2 * chips) % chips
        s = q // (chips // 2)
        return 2 * (q * (1 - s) + (chips - 1 - q) * s) + s

    def device(p):
        return {"dp": 2 * chip_at(p) + 1 - core}

    partner = {"dp": me + 1 - 2 * core}
    mate = {"dp": 2 * (2 * rung + 1 - side) + 1 - core}
    cross = far // 2
    from_middle = ((pos == cross) | (pos == chips - cross), (pos == cross - 1) | (pos == chips - cross - 1))

    def remote(src, dst, send_sem, recv_sem, dev):
        return pltpu.make_async_remote_copy(
            src_ref=src, dst_ref=dst, send_sem=send_sem, recv_sem=recv_sem,
            device_id=dev, device_id_type=pl.DeviceIdType.MESH,
        )

    barrier = pltpu.get_barrier_semaphore()
    for o in range(1, n_sec):
        pl.semaphore_signal(barrier, inc=1, device_id={"section": (sec + o) % n_sec},
                            device_id_type=pl.DeviceIdType.MESH)
    def same(dev):
        return {"dp": dev["dp"] + 2 * core - 1}

    for near in (same(device(pos + 1)), same(device(pos - 1)), partner, same(mate)):
        pl.semaphore_signal(barrier, inc=1, device_id=near, device_id_type=pl.DeviceIdType.MESH)

    kv_cols = pl.ds(pl.multiple_of(2 * hd + core * hd, LANES), hd)
    q_cols = pl.ds(pl.multiple_of(core * hd, LANES), hd)
    wo_rows = pl.ds(pl.multiple_of(core * hd, LANES), hd)
    names = ("secs", "act", "pre", "wkv", "blks", "loss", "acc", "rot", "post", "wo", "wq")
    pairs = [
        (secs_hbm, secs), (act_hbm, act), (pre_hbm, pre), (wkv_hbm.at[0], w.at[:, kv_cols]),
        (blks_hbm, blks), (loss_hbm, loss), (acc_hbm, acc), (rot_hbm, rot), (post_hbm, post),
        (wo_hbm.at[0], wo.at[wo_rows]), (wq_hbm.at[0], w.at[:, q_cols]),
    ]
    loads = {
        name: pltpu.make_async_copy(src, dst, load_sem.at[names.index("wkv") if name in ("wq", "wo") else i])
        for i, (name, (src, dst)) in enumerate(zip(names, pairs))
    }
    for name in ("secs", "act", "blks", "loss", "acc", "pre", "wkv", "wq", "wo", "rot", "post"):
        loads[name].start()

    loads["secs"].wait()
    loads["act"].wait()
    for q in range(n_sec):
        for r in range(act_pp):
            block = act[pick(secs, sec, n_sec, mb, q, r)]
            for k in range(CHUNKS):
                stage[q, k, r] = block[:, k * kd:(k + 1) * kd]
    pl.semaphore_wait(barrier, n_sec - 1 + 4)
    pl.semaphore_signal(ready, inc=1, device_id=partner, device_id_type=pl.DeviceIdType.MESH)
    act_copies = [[] for _ in range(CHUNKS)]
    for k in MIXED:
        for o in range(1, n_sec):
            q = (sec + o) % n_sec
            copy = remote(stage.at[q, k], actrecv[k].at[sec], act_out.at[o - 1], act_sem.at[o - 1, k], {"section": q})
            copy.start()
            act_copies[k].append(copy)
    for k in range(CHUNKS):
        actrecv[k][sec] = stage[sec, k]

    for name in ("acc", "blks", "loss"):
        loads[name].wait()
    term = jnp.full((brows, LANES), loss[0, 0], F32)
    high = term.astype(BF16).astype(F32)
    lane = lax.broadcasted_iota(jnp.int32, (brows, LANES), 1)
    row = lax.broadcasted_iota(jnp.int32, (brows, LANES), 0)
    tail = jnp.where(row > 0, 0.0, jnp.where(lane == 0, high, jnp.where(lane == 1, term - high, 0.0)))

    def pack(p, carry):
        for r in range(blk_pp):
            sacc[p, r, :, pl.ds(0, d)] = acc[pick(blks, me, n_dp, blk, p, r)].astype(BF16)
            sacc[p, r, :, pl.ds(d, LANES)] = tail.astype(BF16)
        return carry

    def pack_near(i, carry):
        j = (i // 2 + 1) % chips
        return pack(2 * chip_at(pos + (j + 1) // 2 * (1 - 2 * (j % 2))) + i % 2, carry)

    other = me + 1 - 2 * core
    step_of = (1, -1)

    def send_block(peer):
        remote(sacc.at[peer], racc.at[me], blk_sem.at[0], blk_sem.at[1], {"dp": peer}).start()

    def send_blocks(places):
        for way, hop in places:
            for c in range(2):
                send_block(2 * chip_at(pos + step_of[way] * hop) + (core + c) % 2)

    lax.fori_loop(0, 4, pack_near, 0)
    pl.semaphore_wait(ready, 1)
    send_blocks([(0, 1), (1, 1)])
    some = n_dp // 16
    lax.fori_loop(4, n_dp - 4 * some, pack_near, 0)
    mine = chips * toks

    def token_at(row, first_core):
        block = row // toks
        j = block % chips
        p = (pos + (j + 1) // 2 * (1 - 2 * (j % 2)) + 2 * chips) % chips
        s = p // (chips // 2)
        return (2 * (2 * (p * (1 - s) + (chips - 1 - p) * s) + s) + (first_core + block // chips + (j + 1) // 2) % 2) * toks + row % toks

    query_token = token_at(lax.broadcasted_iota(jnp.int32, (2 * mine, 1), 0) % mine, core)
    key_token = token_at(lax.broadcasted_iota(jnp.int32, (1, length), 1), 0)
    seen[...] = (key_token <= query_token).astype(F32)

    loads["pre"].wait()

    def hops(way, k):
        return far if (k < CHUNKS // 2) == (way == 0) else far - 1


    def width(k):
        return kd + LANES if k == MIXED[-1] else kd

    def order_at(hop):
        return (MIXED, MIXED) if hop == 1 else AHEAD if hop < far else SORTED

    def await_blocks(columns, sem):
        view = w.at[pl.ds(0, columns * toks // LANES), pl.ds(0, LANES)]
        remote(view, view, sem, sem, partner).wait_recv()

    def place_of(way, hop, k):
        return (hop - 1) * 2 * CHUNKS + (way * CHUNKS + k if hop < far else order_at(hop)[way].index(k))

    def ring_place(way, step, k):
        if step == hops(way, k):
            return (2 * far - 3) * CHUNKS + k
        return (step - 1) * 2 * CHUNKS + (way * CHUNKS if step < far - 1 else 0) + k

    def last(k):
        return 1 if k == MIXED[-1] else 0

    def slot(way, hop):
        return 0 if hop == 0 else min(2 * hop - 1 + way, chips - 1)

    def blocks_of(k, c, slots):
        return gath.at[k, c, slots, :, pl.ds(0, width(k))]

    def gather_copy(way, hop, k):
        return remote(blocks_of(k, core, slot(way, hop - 1)), blocks_of(k, 1 - core, slot(way, hop)),
                      ag_out.at[last(k)], ag_sem.at[place_of(way, hop, k)], device(pos + step_of[way]))

    def forward(way, hop, k):
        if hop < hops(way, k):
            if hop < cross:
                gather_copy(way, hop + 1, k).start()
            else:
                pl.when(jnp.logical_not(from_middle[1 - way]))(gather_copy(way, hop + 1, k).start)
        there = far + 1 - hop
        if cross < there <= hops(1 - way, k):
            across = remote(blocks_of(k, core, slot(way, hop)), blocks_of(k, 1 - core, slot(1 - way, there)),
                            ag_out.at[last(k)], ag_sem.at[place_of(1 - way, there, k)], mate)
            pl.when(from_middle[way])(across.start)

    near = 2 * (far - 2) + 1
    spans = (slice(0, near), slice(near, chips))

    def pass_on(j, k):
        block = blocks_of(k, core, j)
        remote(block, block, fwd_out.at[last(k)], fwd_sem.at[0 if j < near else 1, k % half], partner).start()

    square = jnp.zeros((toks, 1), F32)
    for k in MIXED:
        for copy in act_copies[k]:
            copy.wait_recv()
        owner, number = origin(secs, sec, mb, act_pp, 0)
        piece = actrecv[k][owner, number].astype(F32)
        square = square + jnp.sum(piece * piece, axis=-1, keepdims=True)
        gath[k, core, 0, :, pl.ds(0, kd)] = (piece * pre[:, k * kd:(k + 1) * kd]).astype(BF16)
        if k == MIXED[-1]:
            root = jnp.broadcast_to(lax.rsqrt(square / d + 1e-06), (toks, LANES))
            high = root.astype(BF16).astype(F32)
            lane = lax.broadcasted_iota(jnp.int32, (toks, LANES), 1)
            gath[k, core, 0, :, pl.ds(kd, LANES)] = jnp.where(
                lane == 0, high, jnp.where(lane == 1, root - high, 0.0)).astype(BF16)
        for way in range(2):
            gather_copy(way, 1, k).start()
        pass_on(0, k)


    def project(ks, part_of, fresh):
        span = spans[part_of]
        count = span.stop - span.start

        def add(ref, index, cores, cols):
            terms = sum(
                jnp.dot(gath[k, cores, span, :, pl.ds(0, kd)].reshape(-1, kd), w[k * kd:(k + 1) * kd, cols],
                        preferred_element_type=F32)
                for k in ks
            ).reshape(ref[index].shape)
            ref[index] = terms if fresh else ref[index] + terms

        add(qs, span, core, slice(0, 2 * hd))
        await_blocks(count * sum(width(k) for k in ks), fwd_sem.at[part_of, ks[0] % half])
        add(kvs, (slice(None), span), slice(None), slice(2 * hd, 4 * hd))

    three = w.at[:, pl.ds(0, 3 * hd)]
    weights_loaded = load_sem.at[names.index("wkv")]
    remote(three, three, weights_loaded, weights_loaded, partner).wait_recv()
    two = w.at[:, pl.ds(0, 2 * hd)]
    weights = remote(two, two, w_sem.at[0], w_sem.at[1], partner)
    wo_copy = remote(wo.at[wo_rows], wo.at[wo_rows], w_sem.at[2], w_sem.at[3], partner)

    def share(ref, i):
        remote(ref, ref, w_sem.at[i], w_sem.at[i + 1], partner).start()

    loads["rot"].wait()
    for j in range(chips):
        place = chip_at(pos + (j + 1) // 2 * (1 - 2 * (j % 2)))
        for c in range(2):
            for t in range(2):
                turn[t, c, j] = rot[t, place, (c + (j + 1) // 2) % 2]

    for hop in range(1, far + 1):
        order = order_at(hop)
        for i in range(CHUNKS if hop < far else half):
            if hop == far:
                await_blocks(sum(width(order[way][i]) for way in range(2)), ag_sem.at[place_of(0, hop, order[0][i])])
            for way in range(2):
                k = order[way][i]
                if hop < far:
                    gather_copy(way, hop, k).wait_recv()
                forward(way, hop, k)
                pass_on(slot(way, hop), k)
            if hop == 1:
                rows = pl.ds(i * kd, kd)
                share(w.at[rows, kv_cols], 0)
                share(w.at[rows, q_cols], 0)
                if i < 4:
                    lax.fori_loop(n_dp - (4 - i) * some, n_dp - (3 - i) * some, pack_near, 0)
                elif i == 4:
                    racc[me] = sacc[me]
                    send_block(other)
            if hop == 2:
                share(wo.at[wo_rows, pl.ds(i * kd, kd)], 2)
            if hop == far - 1 and i == CHUNKS - 2:
                send_blocks([(way, far - h) for h in range(1, far - 1) for way in range(2)])
            if hop == far - 1 and i == 1:
                weights.wait_recv()
            if hop == far - 1 and i % 2 == 1:
                project(MIXED[i - 1:i + 1], 0, i == 1)
            if hop == far and i > 0:
                project((i - 1, half + i - 1), 1, i == 1)
            if hop == far and i == 0:
                send_blocks([(0, far)])
    project((half - 1, CHUNKS - 1), 1, False)

    def root_of(parts):
        return jnp.sum(parts.reshape(-1, LANES).astype(F32), axis=-1, keepdims=True)

    def turned(v, tables, root):
        return (v * (tables[0].reshape(-1, hd) * root) + pltpu.roll(v, hd // 2, 1) * (tables[1].reshape(-1, hd) * root)).astype(BF16)

    root = root_of(gath[CHUNKS - 1, :, :, :, pl.ds(kd, LANES)])
    own_root = root_of(gath[CHUNKS - 1, core, :, :, pl.ds(kd, LANES)])
    own_turn = turn[0, core], turn[1, core]

    q_rows = qs[...].reshape(mine, 2 * hd)
    kv_rows = kvs[...].reshape(length, 2 * hd)
    queries = jnp.concatenate([turned(q_rows[:, 0:hd], own_turn, own_root), turned(q_rows[:, hd:2 * hd], own_turn, own_root)], axis=0)
    keys = turned(kv_rows[:, 0:hd], (turn[0], turn[1]), root)
    values = (kv_rows[:, hd:2 * hd] * root).astype(BF16)
    scores = lax.dot_general(queries, keys, (((1,), (1,)), ((), ())), preferred_element_type=F32)
    scores = scores * ((d / n_dp) ** (-0.5) / 50.0)
    expd = jnp.exp(50.0 * jnp.tanh(scores)) * seen[...]
    denominator = jnp.sum(expd, axis=-1, keepdims=True)
    numer = jnp.dot(expd.astype(BF16), values, preferred_element_type=F32)
    attended = (numer / denominator).astype(BF16)
    wo_copy.wait_recv()
    both = jnp.concatenate([attended[0:mine], attended[mine:2 * mine]], axis=1)

    def ring_copy(way, step, k):
        goal = device(pos + step_of[way])
        if hops(way, k) - step + 1 > cross:
            goal = {"dp": jnp.where(from_middle[1 - way], mate["dp"], goal["dp"])}
        return remote(ring_out.at[k, way * far + step - 1], ring_in.at[k, way * far + step - 1],
                      ring_done.at[0], ring_sem.at[ring_place(way, step, k)], goal)

    def crossing(way, step, k):
        return hops(way, k) - step + 1 > cross

    def launch(way, step, k, total):
        ring_out[k, way * far + step - 1] = total.astype(BF16)
        start = ring_copy(way, step, k).start
        if step == 1 and crossing(way, 1, k):
            pl.when(jnp.logical_not(from_middle[1 - way]))(start)
        else:
            start()

    for k in MIXED:
        terms = jnp.dot(both, wo[:, k * kd:(k + 1) * kd], preferred_element_type=F32)
        part[k] = terms.reshape(chips, toks, kd)
        way = 0 if hops(0, k) == far else 1
        launch(way, 1, k, part[k, chips - 1])
    for j in range(half):
        for way in range(2):
            k = SORTED[way][half + j]
            launch(way, 1, k, part[k, slot(1 - way, hops(way, k))])
    for j in range(mb):
        owner, number = origin(secs, sec, mb, act_pp, j)
        for k in range(CHUNKS):
            moved[j, :, k * kd:(k + 1) * kd] = actrecv[k][owner, number]

    def take(way, step, k):
        ring_copy(way, step, k).wait_recv()
        return ring_in[k, way * far + step - 1].astype(F32)

    def relay(way, step, k):
        left = hops(way, k) - step
        target = slot(1 - way, left)
        there = far + 1 - left
        if crossing(way, step, k):
            @pl.when(jnp.logical_not(from_middle[way]))
            def _():
                part[k, target] = part[k, target] + take(way, step, k)
        if cross < there <= hops(1 - way, k):
            @pl.when(from_middle[1 - way])
            def _():
                part[k, target] = part[k, target] + take(1 - way, hops(1 - way, k) - there + 1, k)
        total = part[k, target]
        launch(way, step + 1, k, total if crossing(way, step, k) else total + take(way, step, k))

    for step in range(1, far):
        for group in range(2):
            for j in range(half):
                for way in range(2):
                    k = SORTED[way][group * half + j]
                    if step < hops(way, k):
                        relay(way, step, k)
            if step == 1 and group == 0:
                for way in range(2):
                    for k in SORTED[way][half:] + SORTED[way][:half]:
                        pl.when(from_middle[1 - way])(ring_copy(way, 1, k).start)

    others = pl.ds(0, n_dp - 1)
    all_blocks = remote(sacc.at[others], racc.at[others], blk_sem.at[0], blk_sem.at[1], partner)
    all_blocks.wait_recv()
    scale_sum = jnp.sum(racc[:, 0, :, pl.ds(d, LANES)].astype(F32), axis=0)
    factor = n_dp / jnp.sum(jnp.sum(scale_sum, axis=0, keepdims=True), axis=1, keepdims=True)

    def unpack(b, carry):
        owner, number = origin(blks, me, blk, blk_pp, b)
        accout[b] = racc[owner, number, :, pl.ds(0, d)].astype(F32) * factor
        return carry

    lax.fori_loop(0, blk, unpack, 0)

    loads["post"].wait()
    pieces, square = [None] * CHUNKS, jnp.zeros((toks, 1), F32)
    for k in MIXED:
        await_blocks(2 * kd, ring_sem.at[ring_place(0, hops(0, k), k)])
        total = part[k, 0]
        for way in range(2):
            total = total + ring_in[k, way * far + hops(way, k) - 1].astype(F32)
        pieces[k] = total
        square = square + jnp.sum(total * total, axis=-1, keepdims=True)
    scale = lax.rsqrt(square / d + 1e-06)
    for k in range(CHUNKS):
        cols = slice(k * kd, (k + 1) * kd)
        outbuf[0, :, cols] = (
            moved[0, :, cols].astype(F32) + pieces[k] * scale * post[:, cols]
        ).astype(BF16)
    for copy in (weights, wo_copy, all_blocks):
        copy.wait_send()
    for o in range(1, n_sec):
        q = (sec + o) % n_sec
        remote(stage.at[q], stage.at[q], act_out.at[o - 1], act_sem.at[o - 1, 0], {"section": q}).wait_send()
    for i, span in enumerate((pl.ds(0, CHUNKS - 1), pl.ds(CHUNKS - 1, 1))):
        for slots, sem in ((chips, fwd_out.at[i]), (chips - 1, ag_out.at[i])):
            block = gath.at[span, core, pl.ds(0, slots), :, pl.ds(0, width(i * (CHUNKS - 1)))]
            remote(block, block, sem, fwd_sem.at[0, 0], partner).wait_send()
    block = ring_out.at[:, pl.ds(0, chips - 1)]
    remote(block, block, ring_done.at[0], fwd_sem.at[0, 0], partner).wait_send()


def write_out(moved, accout, outbuf, moved_hbm, newacc_hbm, check_hbm, sems):
    copies = [
        pltpu.make_async_copy(src, dst, sems.at[i])
        for i, (src, dst) in enumerate([(accout, newacc_hbm), (moved, moved_hbm), (outbuf, check_hbm)])
    ]
    for copy in copies:
        copy.start()
    for copy in copies:
        copy.wait()


def make_on_device(n_sec, n_dp):
    def on_device(activations, section_sources, accumulators, block_sources, loss_terms,
                  pre_gain, query_weight, keyval_weight, output_weight, post_gain):
        mb, toks, d = activations.shape
        blk, brows, _ = accumulators.shape
        hd = query_weight.shape[2]
        chips, far, kd, length = n_dp // 2, n_dp // 4, d // CHUNKS, n_dp * toks
        rot = jnp.asarray(rotary_tables(length, hd).reshape(2, chips, 2, toks, hd))
        smem = pltpu.SMEM
        in_hbm = pl.BlockSpec(memory_space=pltpu.HBM)
        vmem = pl.BlockSpec(memory_space=pltpu.VMEM)
        dma = pltpu.SemaphoreType.DMA
        act_pp, blk_pp = mb // n_sec, blk // n_dp
        out_bytes = activations.size * 2 + accumulators.size * 4 + toks * d * 2
        held = pl.pallas_call(
            functools.partial(kernel, (n_sec, n_dp)),
            out_shape=(
                pltpu.VMEM(activations.shape, BF16),
                pltpu.VMEM(accumulators.shape, F32),
                pltpu.VMEM((1, toks, d), BF16),
            ),
            in_specs=[in_hbm] * 11,
            out_specs=(vmem,) * 3,
            scratch_shapes=[
                smem(section_sources.shape, jnp.int32),
                smem(block_sources.shape, jnp.int32),
                smem((1, 1), F32),
                pltpu.VMEM(activations.shape, BF16),
                pltpu.VMEM(accumulators.shape, F32),
                pltpu.VMEM((1, d), F32),
                pltpu.VMEM((1, d), F32),
                pltpu.VMEM(rot.shape, F32),
                pltpu.VMEM((2, 2, chips, toks, hd), F32),
                pltpu.VMEM((length, length), F32),
                pltpu.VMEM((d, 4 * hd), BF16),
                pltpu.VMEM((2 * hd, d), BF16),
                pltpu.VMEM((n_sec, CHUNKS, act_pp, toks, kd), BF16),
                (pltpu.VMEM((n_sec, act_pp, toks, kd), BF16),) * CHUNKS,
                pltpu.VMEM((n_dp, blk_pp, brows, d + LANES), BF16),
                pltpu.VMEM((n_dp, blk_pp, brows, d + LANES), BF16),
                pltpu.VMEM((CHUNKS, 2, chips, toks, kd + LANES), BF16),
                pltpu.VMEM((chips, toks, 2 * hd), F32),
                pltpu.VMEM((2, chips, toks, 2 * hd), F32),
                pltpu.VMEM((CHUNKS, chips, toks, kd), F32),
                pltpu.VMEM((CHUNKS, 2 * far, toks, kd), BF16),
                pltpu.VMEM((CHUNKS, 2 * far, toks, kd), BF16),
                pltpu.SemaphoreType.REGULAR,
                dma((9,)),
                dma((n_sec - 1,)),
                dma((n_sec - 1, CHUNKS)),
                dma((4,)),
                dma((2,)),
                dma((2,)),
                dma((2 * (far - 1) * CHUNKS + CHUNKS // 2,)),
                dma((2,)),
                dma((2, CHUNKS // 2)),
                dma((1,)),
                dma((2 * (far - 1) * CHUNKS,)),
            ],
            compiler_params=pltpu.CompilerParams(
                collective_id=0, has_side_effects=True, vmem_limit_bytes=VMEM_BYTES - 2**16 - out_bytes
            ),
        )(section_sources, block_sources, loss_terms, activations, accumulators,
          pre_gain, query_weight, keyval_weight, output_weight, post_gain, rot)
        return pl.pallas_call(
            write_out,
            out_shape=(
                jax.ShapeDtypeStruct(activations.shape, BF16),
                jax.ShapeDtypeStruct(accumulators.shape, F32),
                jax.ShapeDtypeStruct((1, toks, d), BF16),
            ),
            in_specs=[vmem] * 3,
            out_specs=(in_hbm,) * 3,
            scratch_shapes=[dma((3,))],
            compiler_params=pltpu.CompilerParams(vmem_limit_bytes=4 * 2**20),
        )(*held)

    return on_device


def solution(mesh):
    placed = (
        P("section", "dp", None),
        P(),
        P("dp", "section", None),
        P(),
        P("section", "dp"),
        P("section", None),
        P("section", None, "dp"),
        P("section", None, "dp"),
        P("section", "dp", None),
        P("section", None),
    )
    return jax.shard_map(
        make_on_device(mesh.shape["section"], mesh.shape["dp"]),
        mesh=mesh,
        in_specs=placed,
        out_specs=(P("section", "dp", None), P("dp", "section", None), P("section", "dp", None)),
        check_vma=False,
    )
```
